256 devices in a mesh: gx: 4 (over x), gy: 64 (over y, z, core).
Axes of the slice: x: 4, y: 4, z: 8, core: 2. Of those that a mesh axis runs over, the one named last changes fastest.
Arguments:
- tile_flux: bfloat16 [4, 12, 8, 1048576], P(None, None, None, ('gx', 'gy')), may hold values from -6 to 6
- tile_frac: float32 [8, 1048576], P(None, ('gx', 'gy')), may hold values from 0.02 to 1
- weights: bfloat16 [256, 7, 16, 256, 128], P(('gx', 'gy')), may hold values from -0.049804688 to 0.14941406
- block_row: int32 [256, 7, 16], P(('gx', 'gy')), may hold values from 0 to 47
- block_col: int32 [256, 7, 16], P(('gx', 'gy')), may hold values from 0 to 31
- send_counts: int32 [256, 7], P(('gx', 'gy')), may hold values from 1 to 16, as said below
Outputs:
- atm_flux: float32 [4, 12, 3145728], P(None, None, ('gx', 'gy'))
The draws below stay inside these ranges and needn't reach their ends.
Inputs may be any that keep to these rules, and one draw needn't show every extreme that they name: `send_counts`: live slots of a device at an offset; some device has all 7 offsets at 16, and some device receives 16 live slots from every offset.
All inputs are finite; a program needn't handle non-finite values.
Results may differ from the reference program's by a relative error of at most 0.0029.
Values sent between devices are 32-bit elements; how exact they have to be, the bound alone decides.
A program may use at most 128 MiB of HBM per device.

```python
import math
import jax
import jax.numpy as jnp
from jax import lax

NFLUX = 12
TILES = 8
SUBSTEPS = 4
BROWS = 256
LCOLS = 128
REACH = 3
CAP = 16
LB_DEV = 32
AB_DEV = 48
NOFF = 7
LAND_CELLS = 1048576
ATM_CELLS = 3145728
DEVICES = 256


def draw_send_counts(key, part):
    key_base, key_full = jax.random.split(jax.random.fold_in(key, 17))
    base = jax.random.randint(key_base, (DEVICES, NOFF), 1, CAP // 2 + 1)
    full_dev = jax.random.randint(key_full, (), 0, DEVICES)
    row_ids = jnp.arange(DEVICES, dtype=jnp.int32)[:, None]
    col_ids = jnp.arange(NOFF, dtype=jnp.int32)[None, :]
    source = (full_dev - (col_ids - REACH)) % DEVICES
    filled = (row_ids == full_dev) | (row_ids == source)
    return jnp.where(filled, CAP, base).astype(jnp.int32)


def plant(values, key, least, top_value):
    spot = [jax.random.randint(jax.random.fold_in(key, axis), (), 0, length) for axis, length in enumerate(values.shape)]
    widest = values.shape.index(max(values.shape))
    next_to = spot[:widest] + [(spot[widest] + 1) % values.shape[widest]] + spot[widest + 1:]
    return values.at[tuple(spot)].set(least).at[tuple(next_to)].set(top_value)


def block_scale(own_key, extent, cuts, low, high):
    factor_of = 1.0
    for axis_at, shards_of in cuts:
        steps = jax.random.uniform(jax.random.fold_in(jax.random.fold_in(own_key, 6), axis_at), (shards_of,), jnp.float32, low / len(cuts), high / len(cuts))
        factor_of = factor_of * jnp.repeat(jnp.exp(steps), extent[axis_at] // shards_of).reshape((-1,) + (1,) * (len(extent) - 1 - axis_at))
    return factor_of


def bell_draw(stream_key, extent, spread, bound, cuts=(), held_as=jnp.bfloat16):
    result = spread * jax.random.normal(stream_key, extent, jnp.float32)
    if cuts:
        result = result * block_scale(stream_key, extent, cuts, -0.22, 0.18)
    return jnp.clip(result, -bound, bound).astype(held_as)


def setup_inputs(seed: int = 0) -> dict:
    streams_of = jax.random.split(jax.random.key(seed), 7)
    tile_flux = bell_draw(streams_of[0], (SUBSTEPS, NFLUX, TILES, LAND_CELLS), 1.0, 6.0, ((3, 256),))
    tile_frac = jnp.clip(jnp.exp(math.log(1.0) - 3.912023 * jax.random.uniform(streams_of[1], (TILES, LAND_CELLS), jnp.float32) ** block_scale(streams_of[1], (TILES, LAND_CELLS), ((1, 256),), -0.2, 0.2)), 0.02, 1.0)
    weights = jnp.clip(-0.049804688 + 0.19921875 * jax.random.uniform(streams_of[2], (DEVICES, NOFF, CAP, BROWS, LCOLS), jnp.float32) ** block_scale(streams_of[2], (DEVICES, NOFF, CAP, BROWS, LCOLS), ((0, 256),), -0.2, 0.2), -0.049804688, 0.14941406).astype(jnp.bfloat16)
    block_row = plant(jax.random.randint(streams_of[3], (DEVICES, NOFF, CAP), 0, AB_DEV), jax.random.fold_in(streams_of[3], 1), 0, AB_DEV - 1).astype(jnp.int32)
    block_col = plant(jax.random.randint(streams_of[4], (DEVICES, NOFF, CAP), 0, LB_DEV), jax.random.fold_in(streams_of[4], 1), 0, LB_DEV - 1).astype(jnp.int32)
    send_counts = draw_send_counts(jax.random.fold_in(streams_of[6], 71), 0)
    return {"tile_flux": tile_flux, "tile_frac": tile_frac, "weights": weights, "block_row": block_row, "block_col": block_col, "send_counts": send_counts}


def reference(tile_flux, tile_frac, weights, block_row, block_col, send_counts):
    frac_sum = jnp.sum(tile_frac, axis=0)
    merged = (jnp.sum(tile_flux.astype(jnp.float32) * tile_frac[None, None], axis=2) / frac_sum).astype(jnp.bfloat16)
    width = SUBSTEPS * NFLUX
    land_blocks = merged.reshape(width, DEVICES, LB_DEV, LCOLS).transpose(1, 2, 0, 3)

    def one_device(block_w, columns, counts, blocks):
        picked = blocks[columns]
        partial_value = jnp.einsum('okrc,okfc->okfr', block_w.astype(jnp.float32), picked.astype(jnp.float32))
        active = (jnp.arange(CAP, dtype=jnp.int32)[None, :] < counts[:, None]).astype(jnp.float32)
        return partial_value * active[:, :, None, None]

    def one_group(items):
        return jax.vmap(one_device)(*items)

    group = 8
    grouped = (weights.reshape((DEVICES // group, group) + weights.shape[1:]),
               block_col.reshape((DEVICES // group, group) + block_col.shape[1:]),
               send_counts.reshape((DEVICES // group, group) + send_counts.shape[1:]),
               land_blocks.reshape((DEVICES // group, group) + land_blocks.shape[1:]))
    partials = lax.map(one_group, grouped)
    dest_dev = (jnp.arange(DEVICES, dtype=jnp.int32)[:, None] + jnp.arange(NOFF, dtype=jnp.int32)[None, :] - REACH) % DEVICES
    target = (dest_dev[:, :, None] * AB_DEV + block_row).astype(jnp.int32)
    totals = jnp.zeros((DEVICES * AB_DEV, width, BROWS), jnp.float32)
    totals = totals.at[target.reshape(-1)].add(partials.reshape(-1, width, BROWS))
    return totals.transpose(1, 0, 2).reshape(SUBSTEPS, NFLUX, ATM_CELLS)
```

```python
import functools

import jax
import jax.numpy as jnp
from jax import lax
from jax.experimental import pallas as pl
from jax.experimental.pallas import tpu as pltpu
from jax.sharding import PartitionSpec as P

MESH = pl.DeviceIdType.MESH
AB_DEV = 48
CHUNK = 4
FLUX_CHUNKS = 4


def combine(a, b, shift, mask):
    return jnp.where(mask, a + pltpu.roll(a, 8 - shift, 0), b + pltpu.roll(b, shift, 0))


def sum_rows(parts):
    row = lax.broadcasted_iota(jnp.int32, (8, 128), 0)
    top = [combine(parts[r], parts[r + 4], 4, row < 4) for r in range(4)]
    mid = [combine(top[r], top[r + 2], 2, (row & 2) == 0) for r in range(2)]
    return combine(mid[0], mid[1], 1, (row & 1) == 0)


def send_kernel(
    sizes,
    flux_hbm, frac_hbm, weights_hbm, rows_hbm, col_ref, count_ref,
    arrived_hbm, tables_hbm,
    flux_ref, frac_ref, weights_ref, merged_ref, staged_ref,
    in_sem, weight_sem, own_sem, send_sem, recv_sem, table_send, table_recv,
):
    num_x, num_y = sizes
    devices = num_x * num_y
    num_step, num_kind = flux_ref.shape[:2]
    num_off, slots = weights_ref.shape[:2]
    reach = num_off // 2
    land_blocks = merged_ref.shape[0]
    chunks = slots // CHUNK
    sends = chunks * (num_off - 1)
    wide = flux_ref.shape[3] // FLUX_CHUNKS
    me = lax.axis_index("gx") * num_y + lax.axis_index("gy")

    def flux_copy(part):
        cells = pl.ds(part * wide, wide)
        return pltpu.make_async_copy(
            flux_hbm.at[:, :, :, cells], flux_ref.at[:, :, :, cells], in_sem.at[part]
        )

    def plan(i):
        chunk = i // (num_off - 1)
        turn = i % (num_off - 1)
        off = (reach - turn // 2) * (1 - 2 * (turn % 2))
        return chunk, off

    def weight_copy(chunk, offset, sem):
        part = (offset, pl.ds(chunk * CHUNK, CHUNK))
        return pltpu.make_async_copy(weights_hbm.at[part], weights_ref.at[part], sem)

    def target(off):
        there = (me + off + devices) % devices
        return (there // num_y, there % num_y)

    frac_copy = pltpu.make_async_copy(frac_hbm, frac_ref, in_sem.at[FLUX_CHUNKS])
    frac_copy.start()
    for part in range(FLUX_CHUNKS):
        flux_copy(part).start()

    @pl.loop(0, sends)
    def _(i):
        chunk, off = plan(i)
        weight_copy(chunk, off + reach, weight_sem.at[i]).start()

    @pl.loop(0, chunks)
    def _(chunk):
        weight_copy(chunk, reach, weight_sem.at[sends + chunk]).start()

    barrier = pltpu.get_barrier_semaphore()
    for off in range(-reach, reach + 1):
        if off:
            pl.semaphore_signal(barrier, inc=1, device_id=target(off), device_id_type=MESH)

    frac_copy.wait()

    def merge_block(block):
        cells = pl.ds(pl.multiple_of(block * 128, 128), 128)
        frac = frac_ref[:, cells]
        total = jnp.sum(frac, axis=0, keepdims=True)
        pieces = []
        for first in range(0, num_step * num_kind, 8):
            parts = []
            for line in range(first, first + 8):
                kind, step = line // num_step, line % num_step
                parts.append(flux_ref[step, kind, :, cells].astype(jnp.float32) * frac)
            pieces.append(sum_rows(parts) / total)
        merged_ref[block] = jnp.concatenate(pieces, axis=0).astype(jnp.bfloat16)

    per_part = land_blocks // FLUX_CHUNKS
    for part in range(FLUX_CHUNKS):
        flux_copy(part).wait()
        pl.loop(part * per_part, (part + 1) * per_part)(merge_block)

    pl.semaphore_wait(barrier, num_off - 1)

    def table_copy(off):
        return pltpu.make_async_remote_copy(
            src_ref=rows_hbm,
            dst_ref=tables_hbm.at[off + reach],
            send_sem=table_send.at[off + reach],
            recv_sem=table_recv.at[off + reach],
            device_id=target(off),
            device_id_type=MESH,
        )

    def partial_sums(chunk, offset):
        for step in range(CHUNK):
            slot = chunk * CHUNK + step
            picked = merged_ref[col_ref[offset, slot]]
            picked = jnp.where(slot < count_ref[offset], picked, jnp.zeros_like(picked))
            staged_ref[offset, slot] = lax.dot_general(
                picked, weights_ref[offset, slot], (((1,), (1,)), ((), ())),
                preferred_element_type=jnp.float32,
            )

    def chunk_copy(i):
        chunk, off = plan(i)
        part = (off + reach, pl.ds(chunk * CHUNK, CHUNK))
        return pltpu.make_async_remote_copy(
            src_ref=staged_ref.at[part],
            dst_ref=arrived_hbm.at[part],
            send_sem=send_sem.at[i],
            recv_sem=recv_sem.at[i],
            device_id=target(off),
            device_id_type=MESH,
        )

    @pl.loop(0, sends)
    def _(i):
        chunk, off = plan(i)
        weight_copy(chunk, off + reach, weight_sem.at[i]).wait()
        partial_sums(chunk, off + reach)

        @pl.when(i > 0)
        def _():
            chunk_copy(i - 1).start()

    for off in range(-reach, reach + 1):
        if off:
            table_copy(off).start()
    chunk_copy(sends - 1).start()

    @pl.loop(0, chunks)
    def _(chunk):
        weight_copy(chunk, reach, weight_sem.at[sends + chunk]).wait()
        partial_sums(chunk, reach)

    own = pltpu.make_async_copy(staged_ref.at[reach], arrived_hbm.at[reach], own_sem)
    own.start()
    own_table = pltpu.make_async_copy(rows_hbm, tables_hbm.at[reach], in_sem.at[0])
    own_table.start()

    @pl.loop(0, sends)
    def _(i):
        chunk_copy(i).wait()

    for off in range(-reach, reach + 1):
        if off:
            table_copy(off).wait()
    own.wait()
    own_table.wait()


def settle_kernel(table_ref, arrived_hbm, out_hbm, arrived_ref, total_ref, out_ref, in_sem, out_sem):
    num_off, slots, lines, block_rows = arrived_ref.shape
    num_kind, num_step = out_ref.shape[:2]
    atm_blocks = total_ref.shape[0]
    parts = 4

    def fetch(offset):
        return pltpu.make_async_copy(arrived_hbm.at[offset], arrived_ref.at[offset], in_sem.at[offset])

    for offset in range(num_off):
        fetch(offset).start()

    @pl.loop(0, atm_blocks)
    def _(block):
        total_ref[block] = jnp.zeros((lines, block_rows), jnp.float32)

    for offset in range(num_off):
        fetch(offset).wait()

        @pl.loop(0, slots)
        def _(slot, offset=offset):
            block = table_ref[offset, offset, slot]
            total_ref[block] = total_ref[block] + arrived_ref[offset, slot]

    per_part = atm_blocks // parts

    def emit(part):
        cells = pl.ds(part * per_part * block_rows, per_part * block_rows)
        return pltpu.make_async_copy(out_ref.at[:, :, cells], out_hbm.at[:, :, cells], out_sem.at[part])

    for part in range(parts):

        @pl.loop(part * per_part, (part + 1) * per_part)
        def _(block):
            cells = pl.ds(pl.multiple_of(block * block_rows, block_rows), block_rows)
            for kind in range(num_kind):
                out_ref[kind, :, cells] = total_ref[block, pl.ds(kind * num_step, num_step), :]

        emit(part).start()
    for part in range(parts):
        emit(part).wait()


def on_device(sizes, tile_flux, tile_frac, weights, block_row, block_col, send_counts):
    num_step, num_kind, _, cells = tile_flux.shape
    num_off, slots, block_rows, block_cols = weights.shape[1:]
    lines = num_step * num_kind
    sends = slots // CHUNK * (num_off - 1)
    arrived, tables = pl.pallas_call(
        functools.partial(send_kernel, sizes),
        out_shape=(
            jax.ShapeDtypeStruct((num_off, slots, lines, block_rows), jnp.float32),
            jax.ShapeDtypeStruct((num_off, num_off, slots), jnp.int32),
        ),
        in_specs=[pl.BlockSpec(memory_space=pl.ANY)] * 4
        + [pl.BlockSpec(memory_space=pltpu.SMEM)] * 2,
        out_specs=(pl.BlockSpec(memory_space=pl.ANY), pl.BlockSpec(memory_space=pl.ANY)),
        scratch_shapes=[
            pltpu.VMEM(tile_flux.shape, jnp.bfloat16),
            pltpu.VMEM(tile_frac.shape, jnp.float32),
            pltpu.VMEM(weights.shape[1:], jnp.bfloat16),
            pltpu.VMEM((cells // block_cols, lines, block_cols), jnp.bfloat16),
            pltpu.VMEM((num_off, slots, lines, block_rows), jnp.float32),
            pltpu.SemaphoreType.DMA((FLUX_CHUNKS + 1,)),
            pltpu.SemaphoreType.DMA((slots // CHUNK * num_off,)),
            pltpu.SemaphoreType.DMA,
            pltpu.SemaphoreType.DMA((sends,)),
            pltpu.SemaphoreType.DMA((sends,)),
            pltpu.SemaphoreType.DMA((num_off,)),
            pltpu.SemaphoreType.DMA((num_off,)),
        ],
        compiler_params=pltpu.CompilerParams(
            collective_id=0, has_side_effects=True, vmem_limit_bytes=40 * 1024 * 1024
        ),
    )(tile_flux, tile_frac, weights[0], block_row[0], block_col[0], send_counts[0])
    settled = pl.pallas_call(
        settle_kernel,
        out_shape=jax.ShapeDtypeStruct((num_kind, num_step, AB_DEV * block_rows), jnp.float32),
        in_specs=[pl.BlockSpec(memory_space=pltpu.SMEM), pl.BlockSpec(memory_space=pl.ANY)],
        out_specs=pl.BlockSpec(memory_space=pl.ANY),
        scratch_shapes=[
            pltpu.VMEM((num_off, slots, lines, block_rows), jnp.float32),
            pltpu.VMEM((AB_DEV, lines, block_rows), jnp.float32),
            pltpu.VMEM((num_kind, num_step, AB_DEV * block_rows), jnp.float32),
            pltpu.SemaphoreType.DMA((num_off,)),
            pltpu.SemaphoreType.DMA((4,)),
        ],
        compiler_params=pltpu.CompilerParams(vmem_limit_bytes=24 * 1024 * 1024),
    )(tables, arrived)
    return settled.transpose(1, 0, 2)


def solution(mesh):
    sizes = (mesh.shape["gx"], mesh.shape["gy"])
    return jax.shard_map(
        functools.partial(on_device, sizes),
        mesh=mesh,
        in_specs=(
            P(None, None, None, ("gx", "gy")),
            P(None, ("gx", "gy")),
            P(("gx", "gy"), None, None, None, None),
            P(("gx", "gy"), None, None),
            P(("gx", "gy"), None, None),
            P(("gx", "gy"), None),
        ),
        out_specs=P(None, None, ("gx", "gy")),
        check_vma=False,
    )
```

```python
import functools

import jax
import jax.numpy as jnp
from jax import lax
from jax.experimental import pallas as pl
from jax.experimental.pallas import tpu as pltpu
from jax.sharding import PartitionSpec as P

MESH = pl.DeviceIdType.MESH
AB_DEV = 48
CHUNK = 3
FLUX_CHUNKS = 4


def combine(a, b, shift, mask):
    return jnp.where(mask, a + pltpu.roll(a, 8 - shift, 0), b + pltpu.roll(b, shift, 0))


def sum_rows(parts):
    row = lax.broadcasted_iota(jnp.int32, (8, 128), 0)
    top = [combine(parts[r], parts[r + 4], 4, row < 4) for r in range(4)]
    mid = [combine(top[r], top[r + 2], 2, (row & 2) == 0) for r in range(2)]
    return combine(mid[0], mid[1], 1, (row & 1) == 0)


def send_kernel(
    sizes,
    flux_hbm, frac_hbm, weights_hbm, rows_hbm, col_hbm, count_hbm,
    arrived_hbm, tables_hbm,
    flux_ref, frac_ref, weights_ref, merged_ref, staged_ref, col_ref, count_ref,
    in_sem, first_weight, weight_sem, own_sem, first_send, first_recv, send_sem, recv_sem, table_send, table_recv,
):
    num_x, num_y = sizes
    devices = num_x * num_y
    num_step, num_kind = flux_ref.shape[:2]
    num_off, slots = weights_ref.shape[:2]
    reach = num_off // 2
    others = num_off - 1
    land_blocks = merged_ref.shape[0]
    chunks = (slots - 1) // CHUNK
    sends = chunks * others
    wide = land_blocks // FLUX_CHUNKS
    me = lax.axis_index("gx") * num_y + lax.axis_index("gy")

    def flux_copy(part):
        blocks = pl.ds(part * wide, wide)
        return pltpu.make_async_copy(
            flux_hbm.at[:, :, blocks], flux_ref.at[:, :, blocks], in_sem.at[part]
        )

    def offset_of(turn):
        return (reach - turn // 2) * (1 - 2 * (turn % 2))

    def plan(i):
        return i // others, offset_of(i % others)

    def chunk_part(chunk, offset):
        return offset, pl.ds(1 + chunk * CHUNK, CHUNK)

    def weight_copy(part, sem):
        return pltpu.make_async_copy(weights_hbm.at[part], weights_ref.at[part], sem)

    def first_part(offset):
        return offset, pl.ds(0, 1)

    def target(off):
        there = (me + off + devices) % devices
        return (there // num_y, there % num_y)

    col_copy = pltpu.make_async_copy(col_hbm, col_ref, in_sem.at[FLUX_CHUNKS + 1])
    count_copy = pltpu.make_async_copy(count_hbm, count_ref, in_sem.at[FLUX_CHUNKS + 2])
    frac_copy = pltpu.make_async_copy(frac_hbm, frac_ref, in_sem.at[FLUX_CHUNKS])
    col_copy.start()
    count_copy.start()
    frac_copy.start()
    for part in range(FLUX_CHUNKS):
        flux_copy(part).start()

    barrier = pltpu.get_barrier_semaphore()
    for off in range(-reach, reach + 1):
        if off:
            pl.semaphore_signal(barrier, inc=1, device_id=target(off), device_id_type=MESH)

    for offset in range(num_off):
        weight_copy(first_part(offset), first_weight.at[offset]).start()

    @pl.loop(0, sends)
    def _(i):
        chunk, off = plan(i)
        weight_copy(chunk_part(chunk, off + reach), weight_sem.at[i]).start()

    @pl.loop(0, chunks)
    def _(chunk):
        weight_copy(chunk_part(chunk, reach), weight_sem.at[sends + chunk]).start()

    def merge(block):
        frac = frac_ref[block]
        total = jnp.sum(frac, axis=0, keepdims=True)
        pieces = []
        for first in range(0, num_step * num_kind, 8):
            parts = []
            for line in range(first, first + 8):
                kind, step = line // num_step, line % num_step
                parts.append(flux_ref[step, kind, block].astype(jnp.float32) * frac)
            pieces.append(sum_rows(parts) / total)
        return jnp.concatenate(pieces, axis=0).astype(jnp.bfloat16)

    def table_copy(off):
        return pltpu.make_async_remote_copy(
            src_ref=rows_hbm,
            dst_ref=tables_hbm.at[off + reach],
            send_sem=table_send.at[off + reach],
            recv_sem=table_recv.at[off + reach],
            device_id=target(off),
            device_id_type=MESH,
        )

    def remote(part, off, to_sem, from_sem):
        return pltpu.make_async_remote_copy(
            src_ref=staged_ref.at[part],
            dst_ref=arrived_hbm.at[part],
            send_sem=to_sem,
            recv_sem=from_sem,
            device_id=target(off),
            device_id_type=MESH,
        )

    def first_copy(turn):
        off = offset_of(turn)
        return remote(first_part(off + reach), off, first_send.at[turn], first_recv.at[turn])

    def chunk_copy(i):
        chunk, off = plan(i)
        return remote(chunk_part(chunk, off + reach), off, send_sem.at[i], recv_sem.at[i])

    def multiply(picked, offset, slot):
        picked = jnp.where(slot < count_ref[0, offset], picked, jnp.zeros_like(picked))
        staged_ref[offset, slot] = lax.dot_general(
            picked, weights_ref[offset, slot], (((1,), (1,)), ((), ())),
            preferred_element_type=jnp.float32,
        )

    def multiply_chunk(chunk, offset):
        for step in range(CHUNK):
            slot = 1 + chunk * CHUNK + step
            multiply(merged_ref[col_ref[offset, 0, slot]], offset, slot)

    col_copy.wait()
    count_copy.wait()
    frac_copy.wait()
    for part in range(FLUX_CHUNKS):
        flux_copy(part).wait()
    pl.semaphore_wait(barrier, others)

    @pl.loop(0, others)
    def _(turn):
        offset = offset_of(turn) + reach
        weight_copy(first_part(offset), first_weight.at[offset]).wait()
        multiply(merge(col_ref[offset, 0, 0]), offset, 0)

        @pl.when(turn > 0)
        def _():
            first_copy(turn - 1).start()

    for off in range(-reach, reach + 1):
        if off:
            table_copy(off).start()
    first_copy(others - 1).start()

    @pl.loop(0, land_blocks)
    def _(block):
        merged_ref[block] = merge(block)

    @pl.loop(0, sends)
    def _(i):
        chunk, off = plan(i)
        weight_copy(chunk_part(chunk, off + reach), weight_sem.at[i]).wait()
        multiply_chunk(chunk, off + reach)

        @pl.when(i > 0)
        def _():
            chunk_copy(i - 1).start()

    weight_copy(first_part(reach), first_weight.at[reach]).wait()
    multiply(merged_ref[col_ref[reach, 0, 0]], reach, 0)
    chunk_copy(sends - 1).start()

    @pl.loop(0, chunks)
    def _(chunk):
        weight_copy(chunk_part(chunk, reach), weight_sem.at[sends + chunk]).wait()
        multiply_chunk(chunk, reach)

    own_table = pltpu.make_async_copy(rows_hbm, tables_hbm.at[reach], in_sem.at[0])
    own_table.start()
    own = pltpu.make_async_copy(staged_ref.at[reach], arrived_hbm.at[reach], own_sem)
    own.start()

    @pl.loop(0, others)
    def _(turn):
        first_copy(turn).wait()

    @pl.loop(0, sends)
    def _(i):
        chunk_copy(i).wait()

    for off in range(-reach, reach + 1):
        if off:
            table_copy(off).wait()
    own.wait()
    own_table.wait()


def settle_kernel(table_ref, arrived_ref, out_hbm, total_ref, out_ref, out_sem):
    num_off, slots, lines, block_rows = arrived_ref.shape
    num_kind, num_step = out_ref.shape[:2]
    atm_blocks = total_ref.shape[0]
    parts = 4

    @pl.loop(0, atm_blocks, unroll=4)
    def _(block):
        total_ref[block] = jnp.zeros((lines, block_rows), jnp.float32)

    for offset in range(num_off):

        @pl.loop(0, slots, unroll=4)
        def _(slot, offset=offset):
            block = table_ref[offset, offset, 0, slot]
            total_ref[block] = total_ref[block] + arrived_ref[offset, slot]

    per_part = atm_blocks // parts

    def emit(part):
        cells = pl.ds(part * per_part * block_rows, per_part * block_rows)
        return pltpu.make_async_copy(out_ref.at[:, :, cells], out_hbm.at[:, :, cells], out_sem.at[part])

    for part in range(parts):

        @pl.loop(part * per_part, (part + 1) * per_part, unroll=2)
        def _(block):
            cells = pl.ds(pl.multiple_of(block * block_rows, block_rows), block_rows)
            for kind in range(num_kind):
                out_ref[kind, :, cells] = total_ref[block, pl.ds(kind * num_step, num_step), :]

        emit(part).start()
    for part in range(parts):
        emit(part).wait()


def on_device(sizes, tile_flux, tile_frac, weights, block_row, block_col, send_counts):
    num_step, num_kind, tiles, cells = tile_flux.shape
    num_off, slots, block_rows, block_cols = weights.shape[1:]
    lines = num_step * num_kind
    chunks = (slots - 1) // CHUNK
    sends = chunks * (num_off - 1)
    tile_flux = tile_flux.reshape(num_step, num_kind, tiles, -1, block_cols).transpose(0, 1, 3, 2, 4)
    tile_frac = tile_frac.reshape(tiles, -1, block_cols).transpose(1, 0, 2)
    arrived, tables = pl.pallas_call(
        functools.partial(send_kernel, sizes),
        out_shape=(
            jax.ShapeDtypeStruct((num_off, slots, lines, block_rows), jnp.float32),
            jax.ShapeDtypeStruct((num_off, num_off, 1, slots), jnp.int32),
        ),
        in_specs=[pl.BlockSpec(memory_space=pltpu.HBM)] * 6,
        out_specs=(pl.BlockSpec(memory_space=pl.ANY), pl.BlockSpec(memory_space=pl.ANY)),
        scratch_shapes=[
            pltpu.VMEM(tile_flux.shape, jnp.bfloat16),
            pltpu.VMEM(tile_frac.shape, jnp.float32),
            pltpu.VMEM(weights.shape[1:], jnp.bfloat16),
            pltpu.VMEM((cells // block_cols, lines, block_cols), jnp.bfloat16),
            pltpu.VMEM((num_off, slots, lines, block_rows), jnp.float32),
            pltpu.SMEM((num_off, 1, slots), jnp.int32),
            pltpu.SMEM((1, num_off), jnp.int32),
            pltpu.SemaphoreType.DMA((FLUX_CHUNKS + 3,)),
            pltpu.SemaphoreType.DMA((num_off,)),
            pltpu.SemaphoreType.DMA((chunks * num_off,)),
            pltpu.SemaphoreType.DMA,
            pltpu.SemaphoreType.DMA((num_off - 1,)),
            pltpu.SemaphoreType.DMA((num_off - 1,)),
            pltpu.SemaphoreType.DMA((sends,)),
            pltpu.SemaphoreType.DMA((sends,)),
            pltpu.SemaphoreType.DMA((num_off,)),
            pltpu.SemaphoreType.DMA((num_off,)),
        ],
        compiler_params=pltpu.CompilerParams(
            collective_id=0, has_side_effects=True, vmem_limit_bytes=40 * 1024 * 1024
        ),
    )(*(
        pltpu.with_memory_space_constraint(value, pltpu.HBM)
        for value in (tile_flux, tile_frac, weights[0], block_row.transpose(1, 0, 2), block_col.transpose(1, 0, 2), send_counts)
    ))
    settled = pl.pallas_call(
        settle_kernel,
        out_shape=jax.ShapeDtypeStruct((num_kind, num_step, AB_DEV * block_rows), jnp.float32),
        in_specs=[pl.BlockSpec(memory_space=pltpu.SMEM), pl.BlockSpec(memory_space=pltpu.VMEM)],
        out_specs=pl.BlockSpec(memory_space=pltpu.HBM),
        scratch_shapes=[
            pltpu.VMEM((AB_DEV, lines, block_rows), jnp.float32),
            pltpu.VMEM((num_kind, num_step, AB_DEV * block_rows), jnp.float32),
            pltpu.SemaphoreType.DMA((4,)),
        ],
        compiler_params=pltpu.CompilerParams(vmem_limit_bytes=24 * 1024 * 1024),
    )(tables, arrived)
    return settled.transpose(1, 0, 2)


def solution(mesh):
    sizes = (mesh.shape["gx"], mesh.shape["gy"])
    return jax.shard_map(
        functools.partial(on_device, sizes),
        mesh=mesh,
        in_specs=(
            P(None, None, None, ("gx", "gy")),
            P(None, ("gx", "gy")),
            P(("gx", "gy"), None, None, None, None),
            P(("gx", "gy"), None, None),
            P(("gx", "gy"), None, None),
            P(("gx", "gy"), None),
        ),
        out_specs=P(None, None, ("gx", "gy")),
        check_vma=False,
    )
```

```python
import functools

import jax
import jax.numpy as jnp
from jax import lax
from jax.experimental import pallas as pl
from jax.experimental.pallas import tpu as pltpu
from jax.sharding import PartitionSpec as P

MESH = pl.DeviceIdType.MESH
AB_DEV = 48
CHUNK = 3
PIECE = 8


def combine(a, b, shift, mask):
    return jnp.where(mask, a + pltpu.roll(a, 8 - shift, 0), b + pltpu.roll(b, shift, 0))


def sum_rows(parts):
    row = lax.broadcasted_iota(jnp.int32, (8, 128), 0)
    top = [combine(parts[r], parts[r + 4], 4, row < 4) for r in range(4)]
    mid = [combine(top[r], top[r + 2], 2, (row & 2) == 0) for r in range(2)]
    return combine(mid[0], mid[1], 1, (row & 1) == 0)


def send_kernel(
    sizes,
    flux_hbm, frac_hbm, weights_hbm, rows_hbm, col_hbm, count_hbm,
    late_hbm, total_hbm, tables_hbm,
    flux_refs, frac_ref, weights_ref, merged_ref, staged_ref, arrived_ref, sums_ref, total_ref,
    col_ref, count_ref, table_ref,
    in_sem, first_weight, weight_sem, total_sem, first_send, first_recv, send_sem, recv_sem, table_send, table_recv, ready_sem,
):
    num_x, num_y = sizes
    devices = num_x * num_y
    pieces = len(flux_refs)
    num_step, piece_kinds = flux_refs[0].shape[:2]
    num_kind = pieces * piece_kinds
    num_off, slots = weights_ref.shape[:2]
    reach = num_off // 2
    others = num_off - 1
    land_blocks = merged_ref.shape[0]
    chunks = (slots - 1) // CHUNK
    sends = chunks * others
    early = sends - others
    atm_blocks = sums_ref.shape[0]
    block_rows = staged_ref.shape[3]
    me = lax.axis_index("gx") * num_y + lax.axis_index("gy")

    def flux_copy(piece):
        kinds = pl.ds(piece * piece_kinds, piece_kinds)
        return pltpu.make_async_copy(flux_hbm.at[:, kinds], flux_refs[piece], in_sem.at[piece])

    def offset_of(turn):
        return (reach - turn // 2) * (1 - 2 * (turn % 2))

    def plan(i):
        return i // others, offset_of(i % others)

    def chunk_part(chunk, offset):
        return offset, pl.ds(1 + chunk * CHUNK, CHUNK)

    def weight_copy(part, sem):
        return pltpu.make_async_copy(weights_hbm.at[part], weights_ref.at[part], sem)

    def first_part(offset):
        return offset, pl.ds(0, 1)

    def target(off):
        there = (me + off + devices) % devices
        return (there // num_y, there % num_y)

    col_copy = pltpu.make_async_copy(col_hbm, col_ref, in_sem.at[pieces + 1])
    count_copy = pltpu.make_async_copy(count_hbm, count_ref, in_sem.at[pieces + 2])
    frac_copy = pltpu.make_async_copy(frac_hbm, frac_ref, in_sem.at[pieces])
    col_copy.start()
    count_copy.start()
    frac_copy.start()
    for offset in range(num_off):
        weight_copy(first_part(offset), first_weight.at[offset]).start()
    for piece in range(pieces):
        flux_copy(piece).start()

    barrier = pltpu.get_barrier_semaphore()
    for step in range(1, reach + 1):
        pl.semaphore_signal(barrier, inc=1, device_id=target(-step), device_id_type=MESH)

    def merge_piece(block, piece, frac, total):
        parts = []
        for line in range(PIECE):
            kind, step = line // num_step, line % num_step
            parts.append(flux_refs[piece][step, kind, block].astype(jnp.float32) * frac)
        return sum_rows(parts) / total

    def merge(block):
        frac = frac_ref[block]
        total = jnp.sum(frac, axis=0, keepdims=True)
        return jnp.concatenate(
            [merge_piece(block, piece, frac, total) for piece in range(pieces)], axis=0
        ).astype(jnp.bfloat16)

    def table_copy(off):
        return pltpu.make_async_remote_copy(
            src_ref=rows_hbm.at[off + reach],
            dst_ref=tables_hbm.at[off + reach],
            send_sem=table_send.at[off + reach],
            recv_sem=table_recv.at[off + reach],
            device_id=target(off),
            device_id_type=MESH,
        )

    def remote(part, off, to_sem, from_sem):
        return pltpu.make_async_remote_copy(
            src_ref=staged_ref.at[part],
            dst_ref=arrived_ref.at[part],
            send_sem=to_sem,
            recv_sem=from_sem,
            device_id=target(off),
            device_id_type=MESH,
        )

    def first_copy(turn):
        off = offset_of(turn)
        return remote(first_part(off + reach), off, first_send.at[turn], first_recv.at[turn])

    def chunk_copy(i):
        chunk, off = plan(i)
        return remote(chunk_part(chunk, off + reach), off, send_sem.at[i], recv_sem.at[i])

    def late_copy(turn):
        off = offset_of(turn)
        return pltpu.make_async_remote_copy(
            src_ref=staged_ref.at[chunk_part(chunks - 1, off + reach)],
            dst_ref=late_hbm.at[turn],
            send_sem=send_sem.at[early + turn],
            recv_sem=recv_sem.at[early + turn],
            device_id=target(off),
            device_id_type=MESH,
        )

    def product(picked, offset, slot):
        picked = jnp.where(slot < count_ref[0, offset], picked, jnp.zeros_like(picked))
        return lax.dot_general(
            picked, weights_ref[offset, slot], (((1,), (1,)), ((), ())),
            preferred_element_type=jnp.float32,
        )

    def multiply(picked, offset, slot):
        staged_ref[offset, slot] = product(picked, offset, slot)

    def multiply_chunk(chunk, offset):
        for step in range(CHUNK):
            slot = 1 + chunk * CHUNK + step
            multiply(merged_ref[col_ref[offset, 0, slot]], offset, slot)

    pl.semaphore_wait(barrier, reach)
    for step in range(1, reach + 1):
        pl.semaphore_signal(ready_sem, inc=1, device_id=target(step), device_id_type=MESH)

    col_copy.wait()
    count_copy.wait()
    frac_copy.wait()
    for offset in range(num_off):
        if offset != reach:
            weight_copy(first_part(offset), first_weight.at[offset]).wait()
    for piece in range(pieces):
        flux_copy(piece).wait()
        lines = pl.ds(piece * PIECE, PIECE)
        for off in list(range(reach, 0, -1)) + list(range(-reach, 0)):
            block = col_ref[off + reach, 0, 0]
            frac = frac_ref[block]
            picked = merge_piece(block, piece, frac, jnp.sum(frac, axis=0, keepdims=True))
            staged_ref[off + reach, 0, lines, :] = product(picked.astype(jnp.bfloat16), off + reach, 0)
        for off in range(reach, 0, -1):
            remote(
                (off + reach, 0, lines), off, first_send.at[2 * (reach - off)], first_recv.at[2 * (reach - off)]
            ).start()

    @pl.loop(0, sends)
    def _(i):
        chunk, off = plan(i)
        weight_copy(chunk_part(chunk, off + reach), weight_sem.at[i]).start()

    @pl.loop(0, chunks)
    def _(chunk):
        weight_copy(chunk_part(chunk, reach), weight_sem.at[sends + chunk]).start()

    pl.semaphore_wait(ready_sem, reach)
    for turn in range(1, others, 2):
        first_copy(turn).start()
    for off in range(-reach, reach + 1):
        if off:
            table_copy(off).start()

    @pl.loop(0, land_blocks)
    def _(block):
        merged_ref[block] = merge(block)

    @pl.loop(0, sends)
    def _(i):
        chunk, off = plan(i)
        weight_copy(chunk_part(chunk, off + reach), weight_sem.at[i]).wait()
        multiply_chunk(chunk, off + reach)

        @pl.when(jnp.logical_and(i > 0, i <= early))
        def _():
            chunk_copy(i - 1).start()

        @pl.when(i > early)
        def _():
            late_copy(i - 1 - early).start()

    own_table = pltpu.make_async_copy(rows_hbm.at[reach], tables_hbm.at[reach], in_sem.at[0])
    own_table.start()
    weight_copy(first_part(reach), first_weight.at[reach]).wait()
    multiply(merged_ref[col_ref[reach, 0, 0]], reach, 0)
    late_copy(others - 1).start()

    @pl.loop(0, chunks)
    def _(chunk):
        weight_copy(chunk_part(chunk, reach), weight_sem.at[sends + chunk]).wait()
        multiply_chunk(chunk, reach)

    for off in range(-reach, reach + 1):
        if off:
            table_copy(off).wait()
    own_table.wait()
    all_tables = pltpu.make_async_copy(tables_hbm, table_ref, in_sem.at[1])
    all_tables.start()
    all_tables.wait()

    def accumulate(block, start, slots_in):
        total = start
        for ref, offset, slot in slots_in:
            here = table_ref[offset, 0, slot] == block
            value = ref[offset, slot]
            total = total + jnp.where(here, value, jnp.zeros_like(value))
        sums_ref[block] = total

    @pl.loop(0, atm_blocks)
    def _(block):
        accumulate(
            block,
            jnp.zeros(sums_ref.shape[1:], jnp.float32),
            [(staged_ref, reach, slot) for slot in range(slots)],
        )

    @pl.loop(0, others)
    def _(turn):
        first_copy(turn).wait()

    @pl.loop(0, atm_blocks)
    def _(block):
        accumulate(
            block, sums_ref[block], [(arrived_ref, offset, 0) for offset in range(num_off) if offset != reach]
        )

    @pl.loop(0, chunks - 1)
    def _(chunk):
        @pl.loop(0, others)
        def _(turn):
            chunk_copy(chunk * others + turn).wait_recv()

        @pl.loop(0, atm_blocks)
        def _(block):
            accumulate(
                block,
                sums_ref[block],
                [
                    (arrived_ref, offset, 1 + chunk * CHUNK + step)
                    for offset in range(num_off)
                    if offset != reach
                    for step in range(CHUNK)
                ],
            )

    @pl.loop(0, atm_blocks, unroll=2)
    def _(block):
        cells = pl.ds(pl.multiple_of(block * block_rows, block_rows), block_rows)
        for kind in range(num_kind):
            total_ref[kind, :, cells] = sums_ref[block, pl.ds(kind * num_step, num_step), :]

    total_out = pltpu.make_async_copy(total_ref, total_hbm, total_sem)
    total_out.start()

    @pl.loop(0, early)
    def _(i):
        chunk_copy(i).wait_send()

    total_out.wait()

    @pl.loop(0, others)
    def _(turn):
        late_copy(turn).wait()


def settle_kernel(table_ref, late_ref, total_ref, out_hbm, out_ref, touched_ref, out_sem):
    others, steps, _, block_rows = late_ref.shape
    num_kind, num_step, cells_dev = out_ref.shape
    atm_blocks = cells_dev // block_rows
    reach = others // 2
    first_slot = table_ref.shape[2] - steps

    def cells_of(block):
        return pl.ds(pl.multiple_of(block * block_rows, block_rows), block_rows)

    def emit(ref, block):
        cells = cells_of(block)
        return pltpu.make_async_copy(ref.at[:, :, cells], out_hbm.at[:, :, cells], out_sem)

    arrivals = []
    for turn in range(others):
        offset = (reach - turn // 2) * (1 - 2 * (turn % 2)) + reach
        arrivals += [(turn, step, offset) for step in range(steps)]

    @pl.loop(0, atm_blocks, unroll=8)
    def _(block):
        touched_ref[block] = 0

    for turn, step, offset in arrivals:
        touched_ref[table_ref[offset, 0, first_slot + step]] = 1

    @pl.loop(0, atm_blocks)
    def _(block):
        @pl.when(touched_ref[block] == 0)
        def _():
            emit(total_ref, block).start()

    for turn, step, offset in arrivals:
        block = table_ref[offset, 0, first_slot + step]
        cells = cells_of(block)
        fresh = touched_ref[block] == 1
        touched_ref[block] = 2

        @pl.when(fresh)
        def _():
            for kind in range(num_kind):
                out_ref[kind, :, cells] = (
                    total_ref[kind, :, cells] + late_ref[turn, step, pl.ds(kind * num_step, num_step), :]
                )

        @pl.when(jnp.logical_not(fresh))
        def _():
            for kind in range(num_kind):
                out_ref[kind, :, cells] = (
                    out_ref[kind, :, cells] + late_ref[turn, step, pl.ds(kind * num_step, num_step), :]
                )

    @pl.loop(0, atm_blocks)
    def _(block):
        @pl.when(touched_ref[block] == 2)
        def _():
            emit(out_ref, block).start()

    pltpu.make_async_copy(total_ref, out_hbm, out_sem).wait()


def on_device(sizes, tile_flux, tile_frac, weights, block_row, block_col, send_counts):
    num_step, num_kind, tiles, cells = tile_flux.shape
    num_off, slots, block_rows, block_cols = weights.shape[1:]
    lines = num_step * num_kind
    chunks = (slots - 1) // CHUNK
    sends = chunks * (num_off - 1)
    tile_flux = tile_flux.reshape(num_step, num_kind, tiles, -1, block_cols).transpose(0, 1, 3, 2, 4)
    tile_frac = tile_frac.reshape(tiles, -1, block_cols).transpose(1, 0, 2)
    late, total, tables = pl.pallas_call(
        functools.partial(send_kernel, sizes),
        out_shape=(
            jax.ShapeDtypeStruct((num_off - 1, CHUNK, lines, block_rows), jnp.float32),
            jax.ShapeDtypeStruct((num_kind, num_step, AB_DEV * block_rows), jnp.float32),
            jax.ShapeDtypeStruct((num_off, 1, slots), jnp.int32),
        ),
        in_specs=[pl.BlockSpec(memory_space=pltpu.HBM)] * 6,
        out_specs=(pl.BlockSpec(memory_space=pl.ANY),) * 3,
        scratch_shapes=[
            [pltpu.VMEM((num_step, PIECE // num_step) + tile_flux.shape[2:], jnp.bfloat16)] * (lines // PIECE),
            pltpu.VMEM(tile_frac.shape, jnp.float32),
            pltpu.VMEM(weights.shape[1:], jnp.bfloat16),
            pltpu.VMEM((cells // block_cols, lines, block_cols), jnp.bfloat16),
            pltpu.VMEM((num_off, slots, lines, block_rows), jnp.float32),
            pltpu.VMEM((num_off, slots, lines, block_rows), jnp.float32),
            pltpu.VMEM((AB_DEV, lines, block_rows), jnp.float32),
            pltpu.VMEM((num_kind, num_step, AB_DEV * block_rows), jnp.float32),
            pltpu.SMEM((num_off, 1, slots), jnp.int32),
            pltpu.SMEM((1, num_off), jnp.int32),
            pltpu.SMEM((num_off, 1, slots), jnp.int32),
            pltpu.SemaphoreType.DMA((lines // PIECE + 3,)),
            pltpu.SemaphoreType.DMA((num_off,)),
            pltpu.SemaphoreType.DMA((chunks * num_off,)),
            pltpu.SemaphoreType.DMA,
            pltpu.SemaphoreType.DMA((num_off - 1,)),
            pltpu.SemaphoreType.DMA((num_off - 1,)),
            pltpu.SemaphoreType.DMA((sends,)),
            pltpu.SemaphoreType.DMA((sends,)),
            pltpu.SemaphoreType.DMA((num_off,)),
            pltpu.SemaphoreType.DMA((num_off,)),
            pltpu.SemaphoreType.REGULAR,
        ],
        compiler_params=pltpu.CompilerParams(
            collective_id=0, has_side_effects=True, vmem_limit_bytes=40 * 1024 * 1024
        ),
    )(*(
        pltpu.with_memory_space_constraint(value, pltpu.HBM)
        for value in (tile_flux, tile_frac, weights[0], block_row.transpose(1, 0, 2), block_col.transpose(1, 0, 2), send_counts)
    ))
    settled = pl.pallas_call(
        settle_kernel,
        out_shape=jax.ShapeDtypeStruct((num_kind, num_step, AB_DEV * block_rows), jnp.float32),
        in_specs=[pl.BlockSpec(memory_space=pltpu.SMEM)] + [pl.BlockSpec(memory_space=pltpu.VMEM)] * 2,
        out_specs=pl.BlockSpec(memory_space=pltpu.HBM),
        scratch_shapes=[
            pltpu.VMEM((num_kind, num_step, AB_DEV * block_rows), jnp.float32),
            pltpu.SMEM((AB_DEV,), jnp.int32),
            pltpu.SemaphoreType.DMA,
        ],
        compiler_params=pltpu.CompilerParams(vmem_limit_bytes=12 * 1024 * 1024),
    )(tables, late, total)
    return settled.transpose(1, 0, 2)


def solution(mesh):
    sizes = (mesh.shape["gx"], mesh.shape["gy"])
    return jax.shard_map(
        functools.partial(on_device, sizes),
        mesh=mesh,
        in_specs=(
            P(None, None, None, ("gx", "gy")),
            P(None, ("gx", "gy")),
            P(("gx", "gy"), None, None, None, None),
            P(("gx", "gy"), None, None),
            P(("gx", "gy"), None, None),
            P(("gx", "gy"), None),
        ),
        out_specs=P(None, None, ("gx", "gy")),
        check_vma=False,
    )
```

```python
import functools

import jax
import jax.numpy as jnp
from jax import lax
from jax.experimental import pallas as pl
from jax.experimental.pallas import tpu as pltpu
from jax.sharding import PartitionSpec as P

MESH = pl.DeviceIdType.MESH
AB_DEV = 48
CHUNK = 3
PIECE = 8


def combine(a, b, shift, mask):
    return jnp.where(mask, a + pltpu.roll(a, 8 - shift, 0), b + pltpu.roll(b, shift, 0))


def sum_rows(parts):
    row = lax.broadcasted_iota(jnp.int32, (8, 128), 0)
    top = [combine(parts[r], parts[r + 4], 4, row < 4) for r in range(4)]
    mid = [combine(top[r], top[r + 2], 2, (row & 2) == 0) for r in range(2)]
    return combine(mid[0], mid[1], 1, (row & 1) == 0)


def send_kernel(
    sizes,
    flux_hbm, frac_hbm, weights_hbm, rows_hbm, col_hbm, count_hbm,
    late_hbm, total_hbm, tables_hbm,
    flux_refs, frac_ref, weights_ref, merged_ref, staged_ref, arrived_ref, sums_ref, total_ref,
    col_ref, count_ref, table_ref,
    in_sem, first_weight, weight_sem, total_sem, first_send, first_recv, send_sem, recv_sem, table_send, table_recv, ready_sem,
):
    num_x, num_y = sizes
    devices = num_x * num_y
    pieces = len(flux_refs)
    num_step, piece_kinds = flux_refs[0].shape[:2]
    num_kind = pieces * piece_kinds
    num_off, slots = weights_ref.shape[:2]
    reach = num_off // 2
    others = num_off - 1
    land_blocks = merged_ref.shape[0]
    chunks = (slots - 1) // CHUNK
    sends = chunks * others
    early = sends - others
    atm_blocks = sums_ref.shape[0]
    block_rows = staged_ref.shape[3]
    me = lax.axis_index("gx") * num_y + lax.axis_index("gy")

    def flux_copy(piece):
        kinds = pl.ds(piece * piece_kinds, piece_kinds)
        return pltpu.make_async_copy(flux_hbm.at[:, kinds], flux_refs[piece], in_sem.at[piece])

    def offset_of(turn):
        return (reach - turn // 2) * (1 - 2 * (turn % 2))

    def plan(i):
        return i // others, offset_of(i % others)

    def chunk_part(chunk, offset):
        return offset, pl.ds(1 + chunk * CHUNK, CHUNK)

    def weight_copy(part, sem):
        return pltpu.make_async_copy(weights_hbm.at[part], weights_ref.at[part], sem)

    def first_part(offset):
        return offset, pl.ds(0, 1)

    def rest_copy(offset):
        return weight_copy((offset, pl.ds(1, slots - 1)), weight_sem.at[offset])

    def target(off):
        there = (me + off + devices) % devices
        return (there // num_y, there % num_y)

    col_copy = pltpu.make_async_copy(col_hbm, col_ref, in_sem.at[pieces + 1])
    count_copy = pltpu.make_async_copy(count_hbm, count_ref, in_sem.at[pieces + 2])
    frac_copy = pltpu.make_async_copy(frac_hbm, frac_ref, in_sem.at[pieces])
    col_copy.start()
    count_copy.start()
    frac_copy.start()
    for offset in range(num_off):
        weight_copy(first_part(offset), first_weight.at[offset]).start()
    for piece in range(pieces):
        flux_copy(piece).start()

    barrier = pltpu.get_barrier_semaphore()
    for step in range(1, reach + 1):
        pl.semaphore_signal(barrier, inc=1, device_id=target(-step), device_id_type=MESH)

    def merge_piece(block, piece, frac, total):
        parts = []
        for line in range(PIECE):
            kind, step = line // num_step, line % num_step
            parts.append(flux_refs[piece][step, kind, block].astype(jnp.float32) * frac)
        return sum_rows(parts) / total

    def merge(block):
        frac = frac_ref[block]
        total = jnp.sum(frac, axis=0, keepdims=True)
        return jnp.concatenate(
            [merge_piece(block, piece, frac, total) for piece in range(pieces)], axis=0
        ).astype(jnp.bfloat16)

    def table_copy(off):
        return pltpu.make_async_remote_copy(
            src_ref=rows_hbm.at[off + reach],
            dst_ref=tables_hbm.at[off + reach],
            send_sem=table_send.at[off + reach],
            recv_sem=table_recv.at[off + reach],
            device_id=target(off),
            device_id_type=MESH,
        )

    def remote(part, off, to_sem, from_sem):
        return pltpu.make_async_remote_copy(
            src_ref=staged_ref.at[part],
            dst_ref=arrived_ref.at[part],
            send_sem=to_sem,
            recv_sem=from_sem,
            device_id=target(off),
            device_id_type=MESH,
        )

    def first_copy(turn):
        off = offset_of(turn)
        return remote(first_part(off + reach), off, first_send.at[turn], first_recv.at[turn])

    def chunk_copy(i):
        chunk, off = plan(i)
        return remote(chunk_part(chunk, off + reach), off, send_sem.at[i], recv_sem.at[i])

    def late_copy(turn):
        off = offset_of(turn)
        return pltpu.make_async_remote_copy(
            src_ref=staged_ref.at[chunk_part(chunks - 1, off + reach)],
            dst_ref=late_hbm.at[turn],
            send_sem=send_sem.at[early + turn],
            recv_sem=recv_sem.at[early + turn],
            device_id=target(off),
            device_id_type=MESH,
        )

    def product(picked, offset, slot):
        picked = jnp.where(slot < count_ref[0, offset], picked, jnp.zeros_like(picked))
        return lax.dot_general(
            picked, weights_ref[offset, slot], (((1,), (1,)), ((), ())),
            preferred_element_type=jnp.float32,
        )

    def multiply(picked, offset, slot):
        staged_ref[offset, slot] = product(picked, offset, slot)

    def multiply_chunk(chunk, offset):
        for step in range(CHUNK):
            slot = 1 + chunk * CHUNK + step
            multiply(merged_ref[col_ref[offset, 0, slot]], offset, slot)

    pl.semaphore_wait(barrier, reach)
    for step in range(1, reach + 1):
        pl.semaphore_signal(ready_sem, inc=1, device_id=target(step), device_id_type=MESH)

    col_copy.wait()
    count_copy.wait()
    frac_copy.wait()
    for offset in range(num_off):
        if offset != reach:
            weight_copy(first_part(offset), first_weight.at[offset]).wait()
    for piece in range(pieces):
        flux_copy(piece).wait()
        lines = pl.ds(piece * PIECE, PIECE)
        for off in list(range(reach, 0, -1)) + list(range(-reach, 0)):
            block = col_ref[off + reach, 0, 0]
            frac = frac_ref[block]
            picked = merge_piece(block, piece, frac, jnp.sum(frac, axis=0, keepdims=True))
            staged_ref[off + reach, 0, lines, :] = product(picked.astype(jnp.bfloat16), off + reach, 0)
        for off in range(reach, 0, -1):
            remote(
                (off + reach, 0, lines), off, first_send.at[2 * (reach - off)], first_recv.at[2 * (reach - off)]
            ).start()
        if piece == pieces // 2:
            for turn in range(others):
                rest_copy(offset_of(turn) + reach).start()
            rest_copy(reach).start()

    @pl.loop(0, land_blocks)
    def _(block):
        merged_ref[block] = merge(block)

    pl.semaphore_wait(ready_sem, reach)
    for turn in range(1, others, 2):
        first_copy(turn).start()
    for off in range(-reach, reach + 1):
        if off:
            table_copy(off).start()

    @pl.loop(0, sends)
    def _(i):
        chunk, off = plan(i)

        @pl.when(i < others)
        def _():
            rest_copy(off + reach).wait()

        multiply_chunk(chunk, off + reach)

        @pl.when(jnp.logical_and(i > 0, i <= early))
        def _():
            chunk_copy(i - 1).start()

        @pl.when(i > early)
        def _():
            late_copy(i - 1 - early).start()

    own_table = pltpu.make_async_copy(rows_hbm.at[reach], tables_hbm.at[reach], in_sem.at[0])
    own_table.start()
    weight_copy(first_part(reach), first_weight.at[reach]).wait()
    multiply(merged_ref[col_ref[reach, 0, 0]], reach, 0)
    late_copy(others - 1).start()

    rest_copy(reach).wait()

    @pl.loop(0, chunks)
    def _(chunk):
        multiply_chunk(chunk, reach)

    for off in range(-reach, reach + 1):
        if off:
            table_copy(off).wait()
    own_table.wait()
    all_tables = pltpu.make_async_copy(tables_hbm, table_ref, in_sem.at[1])
    all_tables.start()
    all_tables.wait()

    def accumulate(block, start, slots_in):
        total = start
        for ref, offset, slot in slots_in:
            here = table_ref[offset, 0, slot] == block
            value = ref[offset, slot]
            total = total + jnp.where(here, value, jnp.zeros_like(value))
        sums_ref[block] = total

    @pl.loop(0, atm_blocks)
    def _(block):
        accumulate(
            block,
            jnp.zeros(sums_ref.shape[1:], jnp.float32),
            [(staged_ref, reach, slot) for slot in range(slots)],
        )

    @pl.loop(0, others)
    def _(turn):
        first_copy(turn).wait()

    @pl.loop(0, atm_blocks)
    def _(block):
        accumulate(
            block, sums_ref[block], [(arrived_ref, offset, 0) for offset in range(num_off) if offset != reach]
        )

    @pl.loop(0, chunks - 1)
    def _(chunk):
        @pl.loop(0, others)
        def _(turn):
            chunk_copy(chunk * others + turn).wait_recv()

        @pl.loop(0, atm_blocks)
        def _(block):
            accumulate(
                block,
                sums_ref[block],
                [
                    (arrived_ref, offset, 1 + chunk * CHUNK + step)
                    for offset in range(num_off)
                    if offset != reach
                    for step in range(CHUNK)
                ],
            )

    @pl.loop(0, atm_blocks, unroll=2)
    def _(block):
        cells = pl.ds(pl.multiple_of(block * block_rows, block_rows), block_rows)
        for kind in range(num_kind):
            total_ref[kind, :, cells] = sums_ref[block, pl.ds(kind * num_step, num_step), :]

    total_out = pltpu.make_async_copy(total_ref, total_hbm, total_sem)
    total_out.start()

    @pl.loop(0, early)
    def _(i):
        chunk_copy(i).wait_send()

    total_out.wait()

    @pl.loop(0, others)
    def _(turn):
        late_copy(turn).wait()


def settle_kernel(table_ref, late_ref, total_ref, out_hbm, out_ref, touched_ref, out_sem):
    others, steps, _, block_rows = late_ref.shape
    num_kind, num_step, cells_dev = out_ref.shape
    atm_blocks = cells_dev // block_rows
    reach = others // 2
    first_slot = table_ref.shape[2] - steps

    def cells_of(block):
        return pl.ds(pl.multiple_of(block * block_rows, block_rows), block_rows)

    def emit(ref, block):
        cells = cells_of(block)
        return pltpu.make_async_copy(ref.at[:, :, cells], out_hbm.at[:, :, cells], out_sem)

    arrivals = []
    for turn in range(others):
        offset = (reach - turn // 2) * (1 - 2 * (turn % 2)) + reach
        arrivals += [(turn, step, offset) for step in range(steps)]

    @pl.loop(0, atm_blocks, unroll=8)
    def _(block):
        touched_ref[block] = 0

    for turn, step, offset in arrivals:
        touched_ref[table_ref[offset, 0, first_slot + step]] = 1

    @pl.loop(0, atm_blocks)
    def _(block):
        @pl.when(touched_ref[block] == 0)
        def _():
            emit(total_ref, block).start()

    for turn, step, offset in arrivals:
        block = table_ref[offset, 0, first_slot + step]
        cells = cells_of(block)
        fresh = touched_ref[block] == 1
        touched_ref[block] = 2

        @pl.when(fresh)
        def _():
            for kind in range(num_kind):
                out_ref[kind, :, cells] = (
                    total_ref[kind, :, cells] + late_ref[turn, step, pl.ds(kind * num_step, num_step), :]
                )

        @pl.when(jnp.logical_not(fresh))
        def _():
            for kind in range(num_kind):
                out_ref[kind, :, cells] = (
                    out_ref[kind, :, cells] + late_ref[turn, step, pl.ds(kind * num_step, num_step), :]
                )

    @pl.loop(0, atm_blocks)
    def _(block):
        @pl.when(touched_ref[block] == 2)
        def _():
            emit(out_ref, block).start()

    pltpu.make_async_copy(total_ref, out_hbm, out_sem).wait()


def on_device(sizes, tile_flux, tile_frac, weights, block_row, block_col, send_counts):
    num_step, num_kind, tiles, cells = tile_flux.shape
    num_off, slots, block_rows, block_cols = weights.shape[1:]
    lines = num_step * num_kind
    chunks = (slots - 1) // CHUNK
    sends = chunks * (num_off - 1)
    tile_flux = tile_flux.reshape(num_step, num_kind, tiles, -1, block_cols).transpose(0, 1, 3, 2, 4)
    tile_frac = tile_frac.reshape(tiles, -1, block_cols).transpose(1, 0, 2)
    late, total, tables = pl.pallas_call(
        functools.partial(send_kernel, sizes),
        out_shape=(
            jax.ShapeDtypeStruct((num_off - 1, CHUNK, lines, block_rows), jnp.float32),
            jax.ShapeDtypeStruct((num_kind, num_step, AB_DEV * block_rows), jnp.float32),
            jax.ShapeDtypeStruct((num_off, 1, slots), jnp.int32),
        ),
        in_specs=[pl.BlockSpec(memory_space=pltpu.HBM)] * 6,
        out_specs=(pl.BlockSpec(memory_space=pl.ANY),) * 3,
        scratch_shapes=[
            [pltpu.VMEM((num_step, PIECE // num_step) + tile_flux.shape[2:], jnp.bfloat16)] * (lines // PIECE),
            pltpu.VMEM(tile_frac.shape, jnp.float32),
            pltpu.VMEM(weights.shape[1:], jnp.bfloat16),
            pltpu.VMEM((cells // block_cols, lines, block_cols), jnp.bfloat16),
            pltpu.VMEM((num_off, slots, lines, block_rows), jnp.float32),
            pltpu.VMEM((num_off, slots, lines, block_rows), jnp.float32),
            pltpu.VMEM((AB_DEV, lines, block_rows), jnp.float32),
            pltpu.VMEM((num_kind, num_step, AB_DEV * block_rows), jnp.float32),
            pltpu.SMEM((num_off, 1, slots), jnp.int32),
            pltpu.SMEM((1, num_off), jnp.int32),
            pltpu.SMEM((num_off, 1, slots), jnp.int32),
            pltpu.SemaphoreType.DMA((lines // PIECE + 3,)),
            pltpu.SemaphoreType.DMA((num_off,)),
            pltpu.SemaphoreType.DMA((num_off,)),
            pltpu.SemaphoreType.DMA,
            pltpu.SemaphoreType.DMA((num_off - 1,)),
            pltpu.SemaphoreType.DMA((num_off - 1,)),
            pltpu.SemaphoreType.DMA((sends,)),
            pltpu.SemaphoreType.DMA((sends,)),
            pltpu.SemaphoreType.DMA((num_off,)),
            pltpu.SemaphoreType.DMA((num_off,)),
            pltpu.SemaphoreType.REGULAR,
        ],
        compiler_params=pltpu.CompilerParams(
            collective_id=0, has_side_effects=True, vmem_limit_bytes=40 * 1024 * 1024
        ),
    )(*(
        pltpu.with_memory_space_constraint(value, pltpu.HBM)
        for value in (tile_flux, tile_frac, weights[0], block_row.transpose(1, 0, 2), block_col.transpose(1, 0, 2), send_counts)
    ))
    settled = pl.pallas_call(
        settle_kernel,
        out_shape=jax.ShapeDtypeStruct((num_kind, num_step, AB_DEV * block_rows), jnp.float32),
        in_specs=[pl.BlockSpec(memory_space=pltpu.SMEM)] + [pl.BlockSpec(memory_space=pltpu.VMEM)] * 2,
        out_specs=pl.BlockSpec(memory_space=pltpu.HBM),
        scratch_shapes=[
            pltpu.VMEM((num_kind, num_step, AB_DEV * block_rows), jnp.float32),
            pltpu.SMEM((AB_DEV,), jnp.int32),
            pltpu.SemaphoreType.DMA,
        ],
        compiler_params=pltpu.CompilerParams(vmem_limit_bytes=12 * 1024 * 1024),
    )(tables, late, total)
    return settled.transpose(1, 0, 2)


def solution(mesh):
    sizes = (mesh.shape["gx"], mesh.shape["gy"])
    return jax.shard_map(
        functools.partial(on_device, sizes),
        mesh=mesh,
        in_specs=(
            P(None, None, None, ("gx", "gy")),
            P(None, ("gx", "gy")),
            P(("gx", "gy"), None, None, None, None),
            P(("gx", "gy"), None, None),
            P(("gx", "gy"), None, None),
            P(("gx", "gy"), None),
        ),
        out_specs=P(None, None, ("gx", "gy")),
        check_vma=False,
    )
```

```python
import functools

import jax
import jax.numpy as jnp
from jax import lax
from jax.experimental import pallas as pl
from jax.experimental.pallas import tpu as pltpu
from jax.sharding import PartitionSpec as P

MESH = pl.DeviceIdType.MESH
AB_DEV = 48
CHUNK = 3
PIECE = 8
COLUMN = 16
RELAYED = 2
HELP_AT = 10


def combine(a, b, shift, mask):
    return jnp.where(mask, a + pltpu.roll(a, 8 - shift, 0), b + pltpu.roll(b, shift, 0))


def sum_rows(parts):
    row = lax.broadcasted_iota(jnp.int32, (8, 128), 0)
    top = [combine(parts[r], parts[r + 4], 4, row < 4) for r in range(4)]
    mid = [combine(top[r], top[r + 2], 2, (row & 2) == 0) for r in range(2)]
    return combine(mid[0], mid[1], 1, (row & 1) == 0)


def send_kernel(
    sizes,
    flux_hbm, frac_hbm, weights_hbm, rows_hbm, col_hbm, count_hbm,
    late_hbm, total_hbm, tables_hbm,
    flux_refs, frac_ref, weights_ref, merged_ref, staged_ref, arrived_ref, sums_ref, total_ref,
    col_ref, count_ref, table_ref,
    in_sem, first_weight, weight_sem, total_sem, first_send, first_recv, send_sem, recv_sem, table_send, table_recv, ready_sem,
    relay_ref, relay_ready, relay_send, relay_recv, pass_send, pass_recv,
):
    num_x, num_y = sizes
    devices = num_x * num_y
    pieces = len(flux_refs)
    num_step, piece_kinds = flux_refs[0].shape[:2]
    num_kind = pieces * piece_kinds
    num_off, slots = weights_ref.shape[:2]
    reach = num_off // 2
    others = num_off - 1
    land_blocks = merged_ref.shape[0]
    chunks = (slots - 1) // CHUNK
    sends = chunks * others
    early = sends - others
    atm_blocks = sums_ref.shape[0]
    block_rows = staged_ref.shape[3]
    me = lax.axis_index("gx") * num_y + lax.axis_index("gy")

    columns = num_y // COLUMN
    my_column = lax.axis_index("gy") // COLUMN
    my_chip = lax.axis_index("gy") % COLUMN // 2
    at_end = my_chip == COLUMN // 2 - 1
    is_source = jnp.logical_and(at_end, my_column == columns - 1)
    is_helper = jnp.logical_and(at_end, my_column < columns - 1)
    is_receiver = jnp.logical_and(my_chip == 0, my_column == 0)
    helpers = columns - 1
    assert helpers == CHUNK

    def flux_copy(piece):
        kinds = pl.ds(piece * piece_kinds, piece_kinds)
        return pltpu.make_async_copy(flux_hbm.at[:, kinds], flux_refs[piece], in_sem.at[piece])

    def offset_of(turn):
        return (reach - turn // 2) * (1 - 2 * (turn % 2))

    def plan(i):
        return i // others, offset_of(i % others)

    def chunk_part(chunk, offset):
        return offset, pl.ds(1 + chunk * CHUNK, CHUNK)

    def weight_copy(part, sem):
        return pltpu.make_async_copy(weights_hbm.at[part], weights_ref.at[part], sem)

    def first_part(offset):
        return offset, pl.ds(0, 1)

    def rest_copy(offset):
        return weight_copy((offset, pl.ds(1, slots - 1)), weight_sem.at[offset])

    def target(off):
        there = (me + off + devices) % devices
        return (there // num_y, there % num_y)

    relay_off = 2
    relay_at = relay_off + reach

    def relay_copy(helper):
        return pltpu.make_async_remote_copy(
            src_ref=staged_ref.at[relay_at, 1 + helper],
            dst_ref=relay_ref,
            send_sem=relay_send.at[helper],
            recv_sem=relay_recv,
            device_id=target(-COLUMN * (helpers - helper)),
            device_id_type=MESH,
        )

    def pass_copy(helper):
        return pltpu.make_async_remote_copy(
            src_ref=relay_ref,
            dst_ref=arrived_ref.at[relay_at, 1 + helper],
            send_sem=pass_send,
            recv_sem=pass_recv.at[helper],
            device_id=target(COLUMN * (helpers - helper) + relay_off),
            device_id_type=MESH,
        )

    col_copy = pltpu.make_async_copy(col_hbm, col_ref, in_sem.at[pieces + 1])
    count_copy = pltpu.make_async_copy(count_hbm, count_ref, in_sem.at[pieces + 2])
    frac_copy = pltpu.make_async_copy(frac_hbm, frac_ref, in_sem.at[pieces])
    col_copy.start()
    count_copy.start()
    frac_copy.start()
    for offset in range(num_off):
        weight_copy(first_part(offset), first_weight.at[offset]).start()
    for piece in range(pieces):
        flux_copy(piece).start()

    barrier = pltpu.get_barrier_semaphore()
    for step in range(1, reach + 1):
        pl.semaphore_signal(barrier, inc=1, device_id=target(-step), device_id_type=MESH)

    @pl.when(is_source)
    def _():
        for helper in range(helpers):
            pl.semaphore_signal(
                barrier, inc=1, device_id=target(-COLUMN * (helpers - helper)), device_id_type=MESH
            )

    @pl.when(is_receiver)
    def _():
        for helper in range(helpers):
            pl.semaphore_signal(
                barrier, inc=1, device_id=target(-relay_off - COLUMN * (helpers - helper)), device_id_type=MESH
            )

    def merge_piece(block, piece, frac, total):
        parts = []
        for line in range(PIECE):
            kind, step = line // num_step, line % num_step
            parts.append(flux_refs[piece][step, kind, block].astype(jnp.float32) * frac)
        return sum_rows(parts) / total

    def merge(block):
        frac = frac_ref[block]
        total = jnp.sum(frac, axis=0, keepdims=True)
        return jnp.concatenate(
            [merge_piece(block, piece, frac, total) for piece in range(pieces)], axis=0
        ).astype(jnp.bfloat16)

    def table_copy(off):
        return pltpu.make_async_remote_copy(
            src_ref=rows_hbm.at[off + reach],
            dst_ref=tables_hbm.at[off + reach],
            send_sem=table_send.at[off + reach],
            recv_sem=table_recv.at[off + reach],
            device_id=target(off),
            device_id_type=MESH,
        )

    def remote(part, off, to_sem, from_sem):
        return pltpu.make_async_remote_copy(
            src_ref=staged_ref.at[part],
            dst_ref=arrived_ref.at[part],
            send_sem=to_sem,
            recv_sem=from_sem,
            device_id=target(off),
            device_id_type=MESH,
        )

    def first_copy(turn):
        off = offset_of(turn)
        return remote(first_part(off + reach), off, first_send.at[turn], first_recv.at[turn])

    def chunk_copy(i):
        chunk, off = plan(i)
        return remote(chunk_part(chunk, off + reach), off, send_sem.at[i], recv_sem.at[i])

    def late_copy(turn):
        off = offset_of(turn)
        return pltpu.make_async_remote_copy(
            src_ref=staged_ref.at[chunk_part(chunks - 1, off + reach)],
            dst_ref=late_hbm.at[turn],
            send_sem=send_sem.at[early + turn],
            recv_sem=recv_sem.at[early + turn],
            device_id=target(off),
            device_id_type=MESH,
        )

    def product(picked, offset, slot):
        picked = jnp.where(slot < count_ref[0, offset], picked, jnp.zeros_like(picked))
        return lax.dot_general(
            picked, weights_ref[offset, slot], (((1,), (1,)), ((), ())),
            preferred_element_type=jnp.float32,
        )

    def multiply(picked, offset, slot):
        staged_ref[offset, slot] = product(picked, offset, slot)

    def multiply_chunk(chunk, offset):
        for step in range(CHUNK):
            slot = 1 + chunk * CHUNK + step
            multiply(merged_ref[col_ref[offset, 0, slot]], offset, slot)

    @pl.when(jnp.logical_not(is_helper))
    def _():
        pl.semaphore_wait(barrier, reach)

    @pl.when(is_helper)
    def _():
        pl.semaphore_wait(barrier, reach + 2)
        pl.semaphore_signal(
            relay_ready, inc=1, device_id=target(COLUMN * (helpers - my_column)), device_id_type=MESH
        )

    for step in range(1, reach + 1):
        pl.semaphore_signal(ready_sem, inc=1, device_id=target(step), device_id_type=MESH)

    col_copy.wait()
    count_copy.wait()
    frac_copy.wait()
    for offset in range(num_off):
        if offset != reach:
            weight_copy(first_part(offset), first_weight.at[offset]).wait()
    for piece in range(pieces):
        flux_copy(piece).wait()
        lines = pl.ds(piece * PIECE, PIECE)
        for off in list(range(reach, 0, -1)) + list(range(-reach, 0)):
            block = col_ref[off + reach, 0, 0]
            frac = frac_ref[block]
            picked = merge_piece(block, piece, frac, jnp.sum(frac, axis=0, keepdims=True))
            staged_ref[off + reach, 0, lines, :] = product(picked.astype(jnp.bfloat16), off + reach, 0)
        for off in range(reach, 0, -1):
            remote(
                (off + reach, 0, lines), off, first_send.at[2 * (reach - off)], first_recv.at[2 * (reach - off)]
            ).start()
        if piece == pieces // 2:
            for turn in range(others):
                rest_copy(offset_of(turn) + reach).start()
            rest_copy(reach).start()

    @pl.loop(0, land_blocks)
    def _(block):
        merged_ref[block] = merge(block)

    pl.semaphore_wait(ready_sem, reach)
    for turn in range(1, others, 2):
        first_copy(turn).start()
    for off in range(-reach, reach + 1):
        if off:
            table_copy(off).start()

    @pl.loop(0, sends)
    def _(i):
        chunk, off = plan(i)

        @pl.when(i < others)
        def _():
            rest_copy(off + reach).wait()

        multiply_chunk(chunk, off + reach)

        relayed = jnp.logical_and(is_source, i == RELAYED + 1)

        @pl.when(jnp.logical_and(jnp.logical_and(i > 0, i <= early), jnp.logical_not(relayed)))
        def _():
            chunk_copy(i - 1).start()

        @pl.when(relayed)
        def _():
            pl.semaphore_wait(relay_ready, helpers)
            for helper in range(helpers):
                relay_copy(helper).start()

        @pl.when(jnp.logical_and(is_helper, i == HELP_AT))
        def _():
            relay_copy(0).wait_recv()
            pass_copy(my_column).start()

        @pl.when(i > early)
        def _():
            late_copy(i - 1 - early).start()

    own_table = pltpu.make_async_copy(rows_hbm.at[reach], tables_hbm.at[reach], in_sem.at[0])
    own_table.start()
    weight_copy(first_part(reach), first_weight.at[reach]).wait()
    multiply(merged_ref[col_ref[reach, 0, 0]], reach, 0)
    late_copy(others - 1).start()

    rest_copy(reach).wait()

    @pl.loop(0, chunks)
    def _(chunk):
        multiply_chunk(chunk, reach)

    for off in range(-reach, reach + 1):
        if off:
            table_copy(off).wait()
    own_table.wait()
    all_tables = pltpu.make_async_copy(tables_hbm, table_ref, in_sem.at[1])
    all_tables.start()
    all_tables.wait()

    def accumulate(block, start, slots_in):
        total = start
        for ref, offset, slot in slots_in:
            here = table_ref[offset, 0, slot] == block
            value = ref[offset, slot]
            total = total + jnp.where(here, value, jnp.zeros_like(value))
        sums_ref[block] = total

    @pl.loop(0, atm_blocks)
    def _(block):
        accumulate(
            block,
            jnp.zeros(sums_ref.shape[1:], jnp.float32),
            [(staged_ref, reach, slot) for slot in range(slots)],
        )

    @pl.loop(0, others)
    def _(turn):
        first_copy(turn).wait()

    @pl.loop(0, atm_blocks)
    def _(block):
        accumulate(
            block, sums_ref[block], [(arrived_ref, offset, 0) for offset in range(num_off) if offset != reach]
        )

    @pl.loop(0, chunks - 1)
    def _(chunk):
        @pl.loop(0, others)
        def _(turn):
            @pl.when(jnp.logical_not(jnp.logical_and(is_receiver, chunk * others + turn == RELAYED)))
            def _():
                chunk_copy(chunk * others + turn).wait_recv()

        @pl.when(jnp.logical_and(is_receiver, chunk == 0))
        def _():
            for helper in range(helpers):
                pass_copy(helper).wait_recv()

        @pl.loop(0, atm_blocks)
        def _(block):
            accumulate(
                block,
                sums_ref[block],
                [
                    (arrived_ref, offset, 1 + chunk * CHUNK + step)
                    for offset in range(num_off)
                    if offset != reach
                    for step in range(CHUNK)
                ],
            )

    @pl.loop(0, atm_blocks, unroll=2)
    def _(block):
        cells = pl.ds(pl.multiple_of(block * block_rows, block_rows), block_rows)
        for kind in range(num_kind):
            total_ref[kind, :, cells] = sums_ref[block, pl.ds(kind * num_step, num_step), :]

    total_out = pltpu.make_async_copy(total_ref, total_hbm, total_sem)
    total_out.start()

    @pl.loop(0, early)
    def _(i):
        @pl.when(jnp.logical_not(jnp.logical_and(is_source, i == RELAYED)))
        def _():
            chunk_copy(i).wait_send()

    @pl.when(is_source)
    def _():
        for helper in range(helpers):
            relay_copy(helper).wait_send()

    @pl.when(is_helper)
    def _():
        pass_copy(my_column).wait_send()

    total_out.wait()

    @pl.loop(0, others)
    def _(turn):
        late_copy(turn).wait()


def settle_kernel(table_ref, late_ref, total_ref, out_hbm, out_ref, touched_ref, out_sem):
    others, steps, _, block_rows = late_ref.shape
    num_kind, num_step, cells_dev = out_ref.shape
    atm_blocks = cells_dev // block_rows
    reach = others // 2
    first_slot = table_ref.shape[2] - steps

    def cells_of(block):
        return pl.ds(pl.multiple_of(block * block_rows, block_rows), block_rows)

    def emit(ref, block):
        cells = cells_of(block)
        return pltpu.make_async_copy(ref.at[:, :, cells], out_hbm.at[:, :, cells], out_sem)

    arrivals = []
    for turn in range(others):
        offset = (reach - turn // 2) * (1 - 2 * (turn % 2)) + reach
        arrivals += [(turn, step, offset) for step in range(steps)]

    @pl.loop(0, atm_blocks, unroll=8)
    def _(block):
        touched_ref[block] = 0

    for turn, step, offset in arrivals:
        touched_ref[table_ref[offset, 0, first_slot + step]] = 1

    @pl.loop(0, atm_blocks)
    def _(block):
        @pl.when(touched_ref[block] == 0)
        def _():
            emit(total_ref, block).start()

    for turn, step, offset in arrivals:
        block = table_ref[offset, 0, first_slot + step]
        cells = cells_of(block)
        fresh = touched_ref[block] == 1
        touched_ref[block] = 2

        @pl.when(fresh)
        def _():
            for kind in range(num_kind):
                out_ref[kind, :, cells] = (
                    total_ref[kind, :, cells] + late_ref[turn, step, pl.ds(kind * num_step, num_step), :]
                )

        @pl.when(jnp.logical_not(fresh))
        def _():
            for kind in range(num_kind):
                out_ref[kind, :, cells] = (
                    out_ref[kind, :, cells] + late_ref[turn, step, pl.ds(kind * num_step, num_step), :]
                )

    @pl.loop(0, atm_blocks)
    def _(block):
        @pl.when(touched_ref[block] == 2)
        def _():
            emit(out_ref, block).start()

    pltpu.make_async_copy(total_ref, out_hbm, out_sem).wait()


def on_device(sizes, tile_flux, tile_frac, weights, block_row, block_col, send_counts):
    num_step, num_kind, tiles, cells = tile_flux.shape
    num_off, slots, block_rows, block_cols = weights.shape[1:]
    lines = num_step * num_kind
    chunks = (slots - 1) // CHUNK
    sends = chunks * (num_off - 1)
    tile_flux = tile_flux.reshape(num_step, num_kind, tiles, -1, block_cols).transpose(0, 1, 3, 2, 4)
    tile_frac = tile_frac.reshape(tiles, -1, block_cols).transpose(1, 0, 2)
    late, total, tables = pl.pallas_call(
        functools.partial(send_kernel, sizes),
        out_shape=(
            jax.ShapeDtypeStruct((num_off - 1, CHUNK, lines, block_rows), jnp.float32),
            jax.ShapeDtypeStruct((num_kind, num_step, AB_DEV * block_rows), jnp.float32),
            jax.ShapeDtypeStruct((num_off, 1, slots), jnp.int32),
        ),
        in_specs=[pl.BlockSpec(memory_space=pltpu.HBM)] * 6,
        out_specs=(pl.BlockSpec(memory_space=pl.ANY),) * 3,
        scratch_shapes=[
            [pltpu.VMEM((num_step, PIECE // num_step) + tile_flux.shape[2:], jnp.bfloat16)] * (lines // PIECE),
            pltpu.VMEM(tile_frac.shape, jnp.float32),
            pltpu.VMEM(weights.shape[1:], jnp.bfloat16),
            pltpu.VMEM((cells // block_cols, lines, block_cols), jnp.bfloat16),
            pltpu.VMEM((num_off, slots, lines, block_rows), jnp.float32),
            pltpu.VMEM((num_off, slots, lines, block_rows), jnp.float32),
            pltpu.VMEM((AB_DEV, lines, block_rows), jnp.float32),
            pltpu.VMEM((num_kind, num_step, AB_DEV * block_rows), jnp.float32),
            pltpu.SMEM((num_off, 1, slots), jnp.int32),
            pltpu.SMEM((1, num_off), jnp.int32),
            pltpu.SMEM((num_off, 1, slots), jnp.int32),
            pltpu.SemaphoreType.DMA((lines // PIECE + 3,)),
            pltpu.SemaphoreType.DMA((num_off,)),
            pltpu.SemaphoreType.DMA((num_off,)),
            pltpu.SemaphoreType.DMA,
            pltpu.SemaphoreType.DMA((num_off - 1,)),
            pltpu.SemaphoreType.DMA((num_off - 1,)),
            pltpu.SemaphoreType.DMA((sends,)),
            pltpu.SemaphoreType.DMA((sends,)),
            pltpu.SemaphoreType.DMA((num_off,)),
            pltpu.SemaphoreType.DMA((num_off,)),
            pltpu.SemaphoreType.REGULAR,
            pltpu.VMEM((lines, block_rows), jnp.float32),
            pltpu.SemaphoreType.REGULAR,
            pltpu.SemaphoreType.DMA((CHUNK,)),
            pltpu.SemaphoreType.DMA,
            pltpu.SemaphoreType.DMA,
            pltpu.SemaphoreType.DMA((CHUNK,)),
        ],
        compiler_params=pltpu.CompilerParams(
            collective_id=0, has_side_effects=True, vmem_limit_bytes=40 * 1024 * 1024
        ),
    )(*(
        pltpu.with_memory_space_constraint(value, pltpu.HBM)
        for value in (tile_flux, tile_frac, weights[0], block_row.transpose(1, 0, 2), block_col.transpose(1, 0, 2), send_counts)
    ))
    settled = pl.pallas_call(
        settle_kernel,
        out_shape=jax.ShapeDtypeStruct((num_kind, num_step, AB_DEV * block_rows), jnp.float32),
        in_specs=[pl.BlockSpec(memory_space=pltpu.SMEM)] + [pl.BlockSpec(memory_space=pltpu.VMEM)] * 2,
        out_specs=pl.BlockSpec(memory_space=pltpu.HBM),
        scratch_shapes=[
            pltpu.VMEM((num_kind, num_step, AB_DEV * block_rows), jnp.float32),
            pltpu.SMEM((AB_DEV,), jnp.int32),
            pltpu.SemaphoreType.DMA,
        ],
        compiler_params=pltpu.CompilerParams(vmem_limit_bytes=12 * 1024 * 1024),
    )(tables, late, total)
    return settled.transpose(1, 0, 2)


def solution(mesh):
    sizes = (mesh.shape["gx"], mesh.shape["gy"])
    return jax.shard_map(
        functools.partial(on_device, sizes),
        mesh=mesh,
        in_specs=(
            P(None, None, None, ("gx", "gy")),
            P(None, ("gx", "gy")),
            P(("gx", "gy"), None, None, None, None),
            P(("gx", "gy"), None, None),
            P(("gx", "gy"), None, None),
            P(("gx", "gy"), None),
        ),
        out_specs=P(None, None, ("gx", "gy")),
        check_vma=False,
    )
```

```python
import functools

import jax
import jax.numpy as jnp
from jax import lax
from jax.experimental import pallas as pl
from jax.experimental.pallas import tpu as pltpu
from jax.sharding import PartitionSpec as P

MESH = pl.DeviceIdType.MESH
AB_DEV = 48
CHUNK = 3
PIECE = 8
COLUMN = 16
RELAYED = 2
HELP_AT = 10


def combine(a, b, shift, mask):
    return jnp.where(mask, a + pltpu.roll(a, 8 - shift, 0), b + pltpu.roll(b, shift, 0))


def sum_rows(parts):
    row = lax.broadcasted_iota(jnp.int32, (8, 128), 0)
    top = [combine(parts[r], parts[r + 4], 4, row < 4) for r in range(4)]
    mid = [combine(top[r], top[r + 2], 2, (row & 2) == 0) for r in range(2)]
    return combine(mid[0], mid[1], 1, (row & 1) == 0)


def send_kernel(
    sizes,
    flux_hbm, frac_hbm, weights_hbm, rows_hbm, col_hbm, count_hbm,
    late_hbm, total_hbm, tables_hbm,
    flux_refs, frac_ref, weights_ref, merged_ref, staged_ref, arrived_ref, sums_ref, total_ref,
    col_ref, count_ref, table_ref, rows_ref, live_rows_ref,
    in_sem, first_weight, weight_sem, total_sem, first_send, first_recv, send_sem, recv_sem, table_send, table_recv, ready_sem,
    relay_ref, relay_ready, relay_send, relay_recv, pass_send, pass_recv,
):
    num_x, num_y = sizes
    devices = num_x * num_y
    pieces = len(flux_refs)
    num_step, piece_kinds = flux_refs[0].shape[:2]
    num_kind = pieces * piece_kinds
    num_off, slots = weights_ref.shape[:2]
    reach = num_off // 2
    others = num_off - 1
    land_blocks = merged_ref.shape[0]
    chunks = (slots - 1) // CHUNK
    sends = chunks * others
    early = sends - others
    atm_blocks = sums_ref.shape[0]
    block_rows = staged_ref.shape[3]
    me = lax.axis_index("gx") * num_y + lax.axis_index("gy")

    columns = num_y // COLUMN
    my_column = lax.axis_index("gy") // COLUMN
    my_chip = lax.axis_index("gy") % COLUMN // 2
    at_end = my_chip == COLUMN // 2 - 1
    is_source = jnp.logical_and(at_end, my_column == columns - 1)
    is_helper = jnp.logical_and(at_end, my_column < columns - 1)
    is_receiver = jnp.logical_and(my_chip == 0, my_column == 0)
    helpers = columns - 1
    assert helpers == CHUNK

    def flux_copy(piece):
        kinds = pl.ds(piece * piece_kinds, piece_kinds)
        return pltpu.make_async_copy(flux_hbm.at[:, kinds], flux_refs[piece], in_sem.at[piece])

    def offset_of(turn):
        return (reach - turn // 2) * (1 - 2 * (turn % 2))

    def plan(i):
        return i // others, offset_of(i % others)

    def chunk_part(chunk, offset):
        return offset, pl.ds(1 + chunk * CHUNK, CHUNK)

    def weight_copy(part, sem):
        return pltpu.make_async_copy(weights_hbm.at[part], weights_ref.at[part], sem)

    def first_part(offset):
        return offset, pl.ds(0, 1)

    def rest_copy(offset):
        return weight_copy((offset, pl.ds(1, slots - 1)), weight_sem.at[offset])

    def target(off):
        there = (me + off + devices) % devices
        return (there // num_y, there % num_y)

    relay_off = 2
    relay_at = relay_off + reach

    def relay_copy(helper):
        return pltpu.make_async_remote_copy(
            src_ref=staged_ref.at[relay_at, 1 + helper],
            dst_ref=relay_ref,
            send_sem=relay_send.at[helper],
            recv_sem=relay_recv,
            device_id=target(-COLUMN * (helpers - helper)),
            device_id_type=MESH,
        )

    def pass_copy(helper):
        return pltpu.make_async_remote_copy(
            src_ref=relay_ref,
            dst_ref=arrived_ref.at[relay_at, 1 + helper],
            send_sem=pass_send,
            recv_sem=pass_recv.at[helper],
            device_id=target(COLUMN * (helpers - helper) + relay_off),
            device_id_type=MESH,
        )

    col_copy = pltpu.make_async_copy(col_hbm, col_ref, in_sem.at[pieces + 1])
    count_copy = pltpu.make_async_copy(count_hbm, count_ref, in_sem.at[pieces + 2])
    frac_copy = pltpu.make_async_copy(frac_hbm, frac_ref, in_sem.at[pieces])
    rows_copy = pltpu.make_async_copy(rows_hbm, rows_ref, in_sem.at[pieces + 3])
    col_copy.start()
    count_copy.start()
    frac_copy.start()
    for offset in range(num_off):
        weight_copy(first_part(offset), first_weight.at[offset]).start()
    for piece in range(pieces):
        flux_copy(piece).start()
    rows_copy.start()

    barrier = pltpu.get_barrier_semaphore()
    for step in range(1, reach + 1):
        pl.semaphore_signal(barrier, inc=1, device_id=target(-step), device_id_type=MESH)

    @pl.when(is_source)
    def _():
        for helper in range(helpers):
            pl.semaphore_signal(
                barrier, inc=1, device_id=target(-COLUMN * (helpers - helper)), device_id_type=MESH
            )

    @pl.when(is_receiver)
    def _():
        for helper in range(helpers):
            pl.semaphore_signal(
                barrier, inc=1, device_id=target(-relay_off - COLUMN * (helpers - helper)), device_id_type=MESH
            )

    def merge_piece(block, piece, frac, total):
        parts = []
        for line in range(PIECE):
            kind, step = line // num_step, line % num_step
            parts.append(flux_refs[piece][step, kind, block].astype(jnp.float32) * frac)
        return sum_rows(parts) / total

    def merge(block):
        frac = frac_ref[block]
        total = jnp.sum(frac, axis=0, keepdims=True)
        return jnp.concatenate(
            [merge_piece(block, piece, frac, total) for piece in range(pieces)], axis=0
        ).astype(jnp.bfloat16)

    def table_copy(off):
        return pltpu.make_async_remote_copy(
            src_ref=live_rows_ref.at[off + reach],
            dst_ref=tables_hbm.at[off + reach],
            send_sem=table_send.at[off + reach],
            recv_sem=table_recv.at[off + reach],
            device_id=target(off),
            device_id_type=MESH,
        )

    def remote(part, off, to_sem, from_sem):
        return pltpu.make_async_remote_copy(
            src_ref=staged_ref.at[part],
            dst_ref=arrived_ref.at[part],
            send_sem=to_sem,
            recv_sem=from_sem,
            device_id=target(off),
            device_id_type=MESH,
        )

    def first_copy(turn):
        off = offset_of(turn)
        return remote(first_part(off + reach), off, first_send.at[turn], first_recv.at[turn])

    def chunk_copy(i):
        chunk, off = plan(i)
        return remote(chunk_part(chunk, off + reach), off, send_sem.at[i], recv_sem.at[i])

    def late_copy(turn):
        off = offset_of(turn)
        return pltpu.make_async_remote_copy(
            src_ref=staged_ref.at[chunk_part(chunks - 1, off + reach)],
            dst_ref=late_hbm.at[turn],
            send_sem=send_sem.at[early + turn],
            recv_sem=recv_sem.at[early + turn],
            device_id=target(off),
            device_id_type=MESH,
        )

    def product(picked, offset, slot):
        picked = jnp.where(slot < count_ref[0, offset], picked, jnp.zeros_like(picked))
        return lax.dot_general(
            picked, weights_ref[offset, slot], (((1,), (1,)), ((), ())),
            preferred_element_type=jnp.float32,
        )

    def multiply(picked, offset, slot):
        staged_ref[offset, slot] = product(picked, offset, slot)

    def multiply_chunk(chunk, offset):
        for step in range(CHUNK):
            slot = 1 + chunk * CHUNK + step
            multiply(merged_ref[col_ref[offset, 0, slot]], offset, slot)

    @pl.when(jnp.logical_not(is_helper))
    def _():
        pl.semaphore_wait(barrier, reach)

    @pl.when(is_helper)
    def _():
        pl.semaphore_wait(barrier, reach + 2)
        pl.semaphore_signal(
            relay_ready, inc=1, device_id=target(COLUMN * (helpers - my_column)), device_id_type=MESH
        )

    for step in range(1, reach + 1):
        pl.semaphore_signal(ready_sem, inc=1, device_id=target(step), device_id_type=MESH)

    col_copy.wait()
    count_copy.wait()
    frac_copy.wait()
    for offset in range(num_off):
        if offset != reach:
            weight_copy(first_part(offset), first_weight.at[offset]).wait()
    for piece in range(pieces):
        flux_copy(piece).wait()
        lines = pl.ds(piece * PIECE, PIECE)
        for off in list(range(reach, 0, -1)) + list(range(-reach, 0)):
            block = col_ref[off + reach, 0, 0]
            frac = frac_ref[block]
            picked = merge_piece(block, piece, frac, jnp.sum(frac, axis=0, keepdims=True))
            staged_ref[off + reach, 0, lines, :] = product(picked.astype(jnp.bfloat16), off + reach, 0)
        for off in range(reach, 0, -1):
            remote(
                (off + reach, 0, lines), off, first_send.at[2 * (reach - off)], first_recv.at[2 * (reach - off)]
            ).start()
        if piece == pieces // 2:
            for turn in range(others):
                rest_copy(offset_of(turn) + reach).start()
            rest_copy(reach).start()

    rows_copy.wait()
    slot_ids = lax.broadcasted_iota(jnp.int32, (1, slots), 1)
    for offset in range(num_off):
        live_rows_ref[offset] = jnp.where(slot_ids < count_ref[0, offset], rows_ref[offset], -1)

    @pl.loop(0, land_blocks)
    def _(block):
        merged_ref[block] = merge(block)

    pl.semaphore_wait(ready_sem, reach)
    for turn in range(1, others, 2):
        first_copy(turn).start()
    for off in range(-reach, reach + 1):
        if off:
            table_copy(off).start()

    @pl.loop(0, sends)
    def _(i):
        chunk, off = plan(i)

        @pl.when(i < others)
        def _():
            rest_copy(off + reach).wait()

        multiply_chunk(chunk, off + reach)

        relayed = jnp.logical_and(is_source, i == RELAYED + 1)

        @pl.when(jnp.logical_and(jnp.logical_and(i > 0, i <= early), jnp.logical_not(relayed)))
        def _():
            chunk_copy(i - 1).start()

        @pl.when(relayed)
        def _():
            pl.semaphore_wait(relay_ready, helpers)
            for helper in range(helpers):
                relay_copy(helper).start()

        @pl.when(jnp.logical_and(is_helper, i == HELP_AT))
        def _():
            relay_copy(0).wait_recv()
            pass_copy(my_column).start()

        @pl.when(i > early)
        def _():
            late_copy(i - 1 - early).start()

    own_table = pltpu.make_async_copy(live_rows_ref.at[reach], tables_hbm.at[reach], in_sem.at[0])
    own_table.start()
    weight_copy(first_part(reach), first_weight.at[reach]).wait()
    multiply(merged_ref[col_ref[reach, 0, 0]], reach, 0)
    late_copy(others - 1).start()

    rest_copy(reach).wait()

    @pl.loop(0, chunks)
    def _(chunk):
        multiply_chunk(chunk, reach)

    for off in range(-reach, reach + 1):
        if off:
            table_copy(off).wait()
    own_table.wait()
    all_tables = pltpu.make_async_copy(tables_hbm, table_ref, in_sem.at[1])
    all_tables.start()
    all_tables.wait()

    def accumulate(block, start, slots_in):
        total = start
        for ref, offset, slot in slots_in:
            here = table_ref[offset, 0, slot] == block
            value = ref[offset, slot]
            total = total + jnp.where(here, value, jnp.zeros_like(value))
        sums_ref[block] = total

    @pl.loop(0, atm_blocks)
    def _(block):
        accumulate(
            block,
            jnp.zeros(sums_ref.shape[1:], jnp.float32),
            [(staged_ref, reach, slot) for slot in range(slots)],
        )

    @pl.loop(0, others)
    def _(turn):
        first_copy(turn).wait()

    @pl.loop(0, atm_blocks)
    def _(block):
        accumulate(
            block, sums_ref[block], [(arrived_ref, offset, 0) for offset in range(num_off) if offset != reach]
        )

    @pl.loop(0, chunks - 1)
    def _(chunk):
        @pl.loop(0, others)
        def _(turn):
            @pl.when(jnp.logical_not(jnp.logical_and(is_receiver, chunk * others + turn == RELAYED)))
            def _():
                chunk_copy(chunk * others + turn).wait_recv()

        @pl.when(jnp.logical_and(is_receiver, chunk == 0))
        def _():
            for helper in range(helpers):
                pass_copy(helper).wait_recv()

        @pl.loop(0, atm_blocks)
        def _(block):
            accumulate(
                block,
                sums_ref[block],
                [
                    (arrived_ref, offset, 1 + chunk * CHUNK + step)
                    for offset in range(num_off)
                    if offset != reach
                    for step in range(CHUNK)
                ],
            )

    @pl.loop(0, atm_blocks, unroll=2)
    def _(block):
        cells = pl.ds(pl.multiple_of(block * block_rows, block_rows), block_rows)
        for kind in range(num_kind):
            total_ref[kind, :, cells] = sums_ref[block, pl.ds(kind * num_step, num_step), :]

    total_out = pltpu.make_async_copy(total_ref, total_hbm, total_sem)
    total_out.start()

    @pl.loop(0, early)
    def _(i):
        @pl.when(jnp.logical_not(jnp.logical_and(is_source, i == RELAYED)))
        def _():
            chunk_copy(i).wait_send()

    @pl.when(is_source)
    def _():
        for helper in range(helpers):
            relay_copy(helper).wait_send()

    @pl.when(is_helper)
    def _():
        pass_copy(my_column).wait_send()

    total_out.wait()

    @pl.loop(0, others)
    def _(turn):
        late_copy(turn).wait()


def settle_kernel(table_ref, late_ref, total_ref, out_hbm, out_ref, touched_ref, out_sem):
    others, steps, _, block_rows = late_ref.shape
    num_kind, num_step, cells_dev = out_ref.shape
    atm_blocks = cells_dev // block_rows
    reach = others // 2
    first_slot = table_ref.shape[2] - steps

    def cells_of(block):
        return pl.ds(pl.multiple_of(block * block_rows, block_rows), block_rows)

    def emit(ref, block):
        cells = cells_of(block)
        return pltpu.make_async_copy(ref.at[:, :, cells], out_hbm.at[:, :, cells], out_sem)

    arrivals = []
    for turn in range(others):
        offset = (reach - turn // 2) * (1 - 2 * (turn % 2)) + reach
        arrivals += [(turn, step, offset) for step in range(steps)]

    live = 0
    for turn, step, offset in arrivals:
        live = live + jnp.where(table_ref[offset, 0, first_slot + step] >= 0, 1, 0)

    @pl.when(live == 0)
    def _():
        pltpu.make_async_copy(total_ref, out_hbm, out_sem).start()

    @pl.when(live > 0)
    def _():
        @pl.loop(0, atm_blocks, unroll=8)
        def _(block):
            touched_ref[block] = 0

        for turn, step, offset in arrivals:
            row = table_ref[offset, 0, first_slot + step]

            @pl.when(row >= 0)
            def _():
                touched_ref[jnp.maximum(row, 0)] = 1

        @pl.loop(0, atm_blocks)
        def _(block):
            @pl.when(touched_ref[block] == 0)
            def _():
                emit(total_ref, block).start()

        for turn, step, offset in arrivals:
            row = table_ref[offset, 0, first_slot + step]

            @pl.when(row >= 0)
            def _():
                block = jnp.maximum(row, 0)
                cells = cells_of(block)
                fresh = touched_ref[block] == 1
                touched_ref[block] = 2

                @pl.when(fresh)
                def _():
                    for kind in range(num_kind):
                        out_ref[kind, :, cells] = (
                            total_ref[kind, :, cells] + late_ref[turn, step, pl.ds(kind * num_step, num_step), :]
                        )

                @pl.when(jnp.logical_not(fresh))
                def _():
                    for kind in range(num_kind):
                        out_ref[kind, :, cells] = (
                            out_ref[kind, :, cells] + late_ref[turn, step, pl.ds(kind * num_step, num_step), :]
                        )

        @pl.loop(0, atm_blocks)
        def _(block):
            @pl.when(touched_ref[block] == 2)
            def _():
                emit(out_ref, block).start()

    pltpu.make_async_copy(total_ref, out_hbm, out_sem).wait()


def on_device(sizes, tile_flux, tile_frac, weights, block_row, block_col, send_counts):
    num_step, num_kind, tiles, cells = tile_flux.shape
    num_off, slots, block_rows, block_cols = weights.shape[1:]
    lines = num_step * num_kind
    chunks = (slots - 1) // CHUNK
    sends = chunks * (num_off - 1)
    tile_flux = tile_flux.reshape(num_step, num_kind, tiles, -1, block_cols).transpose(0, 1, 3, 2, 4)
    tile_frac = tile_frac.reshape(tiles, -1, block_cols).transpose(1, 0, 2)
    late, total, tables = pl.pallas_call(
        functools.partial(send_kernel, sizes),
        out_shape=(
            jax.ShapeDtypeStruct((num_off - 1, CHUNK, lines, block_rows), jnp.float32),
            jax.ShapeDtypeStruct((num_kind, num_step, AB_DEV * block_rows), jnp.float32),
            jax.ShapeDtypeStruct((num_off, 1, slots), jnp.int32),
        ),
        in_specs=[pl.BlockSpec(memory_space=pltpu.HBM)] * 6,
        out_specs=(pl.BlockSpec(memory_space=pl.ANY),) * 3,
        scratch_shapes=[
            [pltpu.VMEM((num_step, PIECE // num_step) + tile_flux.shape[2:], jnp.bfloat16)] * (lines // PIECE),
            pltpu.VMEM(tile_frac.shape, jnp.float32),
            pltpu.VMEM(weights.shape[1:], jnp.bfloat16),
            pltpu.VMEM((cells // block_cols, lines, block_cols), jnp.bfloat16),
            pltpu.VMEM((num_off, slots, lines, block_rows), jnp.float32),
            pltpu.VMEM((num_off, slots, lines, block_rows), jnp.float32),
            pltpu.VMEM((AB_DEV, lines, block_rows), jnp.float32),
            pltpu.VMEM((num_kind, num_step, AB_DEV * block_rows), jnp.float32),
            pltpu.SMEM((num_off, 1, slots), jnp.int32),
            pltpu.SMEM((1, num_off), jnp.int32),
            pltpu.SMEM((num_off, 1, slots), jnp.int32),
            pltpu.VMEM((num_off, 1, slots), jnp.int32),
            pltpu.VMEM((num_off, 1, slots), jnp.int32),
            pltpu.SemaphoreType.DMA((lines // PIECE + 4,)),
            pltpu.SemaphoreType.DMA((num_off,)),
            pltpu.SemaphoreType.DMA((num_off,)),
            pltpu.SemaphoreType.DMA,
            pltpu.SemaphoreType.DMA((num_off - 1,)),
            pltpu.SemaphoreType.DMA((num_off - 1,)),
            pltpu.SemaphoreType.DMA((sends,)),
            pltpu.SemaphoreType.DMA((sends,)),
            pltpu.SemaphoreType.DMA((num_off,)),
            pltpu.SemaphoreType.DMA((num_off,)),
            pltpu.SemaphoreType.REGULAR,
            pltpu.VMEM((lines, block_rows), jnp.float32),
            pltpu.SemaphoreType.REGULAR,
            pltpu.SemaphoreType.DMA((CHUNK,)),
            pltpu.SemaphoreType.DMA,
            pltpu.SemaphoreType.DMA,
            pltpu.SemaphoreType.DMA((CHUNK,)),
        ],
        compiler_params=pltpu.CompilerParams(
            collective_id=0, has_side_effects=True, vmem_limit_bytes=40 * 1024 * 1024
        ),
    )(*(
        pltpu.with_memory_space_constraint(value, pltpu.HBM)
        for value in (tile_flux, tile_frac, weights[0], block_row.transpose(1, 0, 2), block_col.transpose(1, 0, 2), send_counts)
    ))
    settled = pl.pallas_call(
        settle_kernel,
        out_shape=jax.ShapeDtypeStruct((num_kind, num_step, AB_DEV * block_rows), jnp.float32),
        in_specs=[pl.BlockSpec(memory_space=pltpu.SMEM)] + [pl.BlockSpec(memory_space=pltpu.VMEM)] * 2,
        out_specs=pl.BlockSpec(memory_space=pltpu.HBM),
        scratch_shapes=[
            pltpu.VMEM((num_kind, num_step, AB_DEV * block_rows), jnp.float32),
            pltpu.SMEM((AB_DEV,), jnp.int32),
            pltpu.SemaphoreType.DMA,
        ],
        compiler_params=pltpu.CompilerParams(vmem_limit_bytes=12 * 1024 * 1024),
    )(tables, late, total)
    return settled.transpose(1, 0, 2)


def solution(mesh):
    sizes = (mesh.shape["gx"], mesh.shape["gy"])
    return jax.shard_map(
        functools.partial(on_device, sizes),
        mesh=mesh,
        in_specs=(
            P(None, None, None, ("gx", "gy")),
            P(None, ("gx", "gy")),
            P(("gx", "gy"), None, None, None, None),
            P(("gx", "gy"), None, None),
            P(("gx", "gy"), None, None),
            P(("gx", "gy"), None),
        ),
        out_specs=P(None, None, ("gx", "gy")),
        check_vma=False,
    )
```

```python
import functools

import jax
import jax.numpy as jnp
from jax import lax
from jax.experimental import pallas as pl
from jax.experimental.pallas import tpu as pltpu
from jax.sharding import PartitionSpec as P

MESH = pl.DeviceIdType.MESH
AB_DEV = 48
PARTS = 4
CHUNK = 3
PIECE = 8
COLUMN = 16
RELAYED = 2
HELP_AT = 10


def combine(a, b, shift, mask):
    return jnp.where(mask, a + pltpu.roll(a, 8 - shift, 0), b + pltpu.roll(b, shift, 0))


def sum_rows(parts):
    row = lax.broadcasted_iota(jnp.int32, (8, 128), 0)
    top = [combine(parts[r], parts[r + 4], 4, row < 4) for r in range(4)]
    mid = [combine(top[r], top[r + 2], 2, (row & 2) == 0) for r in range(2)]
    return combine(mid[0], mid[1], 1, (row & 1) == 0)


def send_kernel(
    sizes,
    flux_hbm, frac_hbm, weights_hbm, rows_hbm, col_hbm, count_hbm,
    late_hbm, total_hbm, tables_hbm,
    flux_refs, frac_ref, weights_ref, merged_ref, staged_ref, arrived_ref, sums_ref, total_ref,
    col_ref, count_ref, table_ref, rows_ref, live_rows_ref,
    in_sem, first_weight, weight_sem, total_sem, first_send, first_recv, send_sem, recv_sem, table_send, table_recv, ready_sem,
    relay_ref, relay_ready, relay_send, relay_recv, pass_send, pass_recv,
):
    num_x, num_y = sizes
    devices = num_x * num_y
    pieces = len(flux_refs)
    num_step, piece_kinds = flux_refs[0].shape[:2]
    num_kind = pieces * piece_kinds
    num_off, slots = weights_ref.shape[:2]
    reach = num_off // 2
    others = num_off - 1
    land_blocks = merged_ref.shape[0]
    chunks = (slots - 1) // CHUNK
    sends = chunks * others
    early = sends - others
    atm_blocks = sums_ref.shape[0]
    block_rows = staged_ref.shape[3]
    me = lax.axis_index("gx") * num_y + lax.axis_index("gy")

    columns = num_y // COLUMN
    my_column = lax.axis_index("gy") // COLUMN
    my_chip = lax.axis_index("gy") % COLUMN // 2
    at_end = my_chip == COLUMN // 2 - 1
    is_source = jnp.logical_and(at_end, my_column == columns - 1)
    is_helper = jnp.logical_and(at_end, my_column < columns - 1)
    is_receiver = jnp.logical_and(my_chip == 0, my_column == 0)
    helpers = columns - 1
    assert helpers == CHUNK

    def flux_copy(piece):
        kinds = pl.ds(piece * piece_kinds, piece_kinds)
        return pltpu.make_async_copy(flux_hbm.at[:, kinds], flux_refs[piece], in_sem.at[piece])

    def offset_of(turn):
        return (reach - turn // 2) * (1 - 2 * (turn % 2))

    def plan(i):
        return i // others, offset_of(i % others)

    def chunk_part(chunk, offset):
        return offset, pl.ds(1 + chunk * CHUNK, CHUNK)

    def weight_copy(part, sem):
        return pltpu.make_async_copy(weights_hbm.at[part], weights_ref.at[part], sem)

    def first_part(offset):
        return offset, pl.ds(0, 1)

    def rest_copy(offset):
        return weight_copy((offset, pl.ds(1, slots - 1)), weight_sem.at[offset])

    def target(off):
        there = (me + off + devices) % devices
        return (there // num_y, there % num_y)

    relay_off = 2
    relay_at = relay_off + reach

    def relay_copy(helper):
        return pltpu.make_async_remote_copy(
            src_ref=staged_ref.at[relay_at, 1 + helper],
            dst_ref=relay_ref,
            send_sem=relay_send.at[helper],
            recv_sem=relay_recv,
            device_id=target(-COLUMN * (helpers - helper)),
            device_id_type=MESH,
        )

    def pass_copy(helper):
        return pltpu.make_async_remote_copy(
            src_ref=relay_ref,
            dst_ref=arrived_ref.at[relay_at, 1 + helper],
            send_sem=pass_send,
            recv_sem=pass_recv.at[helper],
            device_id=target(COLUMN * (helpers - helper) + relay_off),
            device_id_type=MESH,
        )

    barrier = pltpu.get_barrier_semaphore()
    for step in range(1, reach + 1):
        pl.semaphore_signal(barrier, inc=1, device_id=target(-step), device_id_type=MESH)

    @pl.when(is_source)
    def _():
        for helper in range(helpers):
            pl.semaphore_signal(
                barrier, inc=1, device_id=target(-COLUMN * (helpers - helper)), device_id_type=MESH
            )

    @pl.when(is_receiver)
    def _():
        for helper in range(helpers):
            pl.semaphore_signal(
                barrier, inc=1, device_id=target(-relay_off - COLUMN * (helpers - helper)), device_id_type=MESH
            )

    col_copy = pltpu.make_async_copy(col_hbm, col_ref, in_sem.at[pieces + 1])
    count_copy = pltpu.make_async_copy(count_hbm, count_ref, in_sem.at[pieces + 2])
    frac_copy = pltpu.make_async_copy(frac_hbm, frac_ref, in_sem.at[pieces])
    rows_copy = pltpu.make_async_copy(rows_hbm, rows_ref, in_sem.at[pieces + 3])
    col_copy.start()
    count_copy.start()
    frac_copy.start()
    for offset in range(num_off):
        weight_copy(first_part(offset), first_weight.at[offset]).start()
    for piece in range(pieces):
        flux_copy(piece).start()
    rows_copy.start()

    def merge_piece(block, piece, frac, total):
        parts = []
        for line in range(PIECE):
            kind, step = line // num_step, line % num_step
            parts.append(flux_refs[piece][step, kind, block].astype(jnp.float32) * frac)
        return sum_rows(parts) / total

    def merge(block):
        frac = frac_ref[block]
        total = jnp.sum(frac, axis=0, keepdims=True)
        return jnp.concatenate(
            [merge_piece(block, piece, frac, total) for piece in range(pieces)], axis=0
        ).astype(jnp.bfloat16)

    def table_copy(off):
        return pltpu.make_async_remote_copy(
            src_ref=live_rows_ref.at[off + reach],
            dst_ref=tables_hbm.at[off + reach],
            send_sem=table_send.at[off + reach],
            recv_sem=table_recv.at[off + reach],
            device_id=target(off),
            device_id_type=MESH,
        )

    def remote(part, off, to_sem, from_sem):
        return pltpu.make_async_remote_copy(
            src_ref=staged_ref.at[part],
            dst_ref=arrived_ref.at[part],
            send_sem=to_sem,
            recv_sem=from_sem,
            device_id=target(off),
            device_id_type=MESH,
        )

    def first_copy(turn):
        off = offset_of(turn)
        return remote(first_part(off + reach), off, first_send.at[turn], first_recv.at[turn])

    def chunk_copy(i):
        chunk, off = plan(i)
        return remote(chunk_part(chunk, off + reach), off, send_sem.at[i], recv_sem.at[i])

    def late_copy(turn):
        off = offset_of(turn)
        return pltpu.make_async_remote_copy(
            src_ref=staged_ref.at[chunk_part(chunks - 1, off + reach)],
            dst_ref=late_hbm.at[turn],
            send_sem=send_sem.at[early + turn],
            recv_sem=recv_sem.at[early + turn],
            device_id=target(off),
            device_id_type=MESH,
        )

    def product(picked, offset, slot):
        picked = jnp.where(slot < count_ref[0, offset], picked, jnp.zeros_like(picked))
        return lax.dot_general(
            picked, weights_ref[offset, slot], (((1,), (1,)), ((), ())),
            preferred_element_type=jnp.float32,
        )

    def multiply(picked, offset, slot):
        staged_ref[offset, slot] = product(picked, offset, slot)

    def multiply_chunk(chunk, offset):
        for step in range(CHUNK):
            slot = 1 + chunk * CHUNK + step
            multiply(merged_ref[col_ref[offset, 0, slot]], offset, slot)

    @pl.when(jnp.logical_not(is_helper))
    def _():
        pl.semaphore_wait(barrier, reach)

    @pl.when(is_helper)
    def _():
        pl.semaphore_wait(barrier, reach + 2)
        pl.semaphore_signal(
            relay_ready, inc=1, device_id=target(COLUMN * (helpers - my_column)), device_id_type=MESH
        )

    for step in range(1, reach + 1):
        pl.semaphore_signal(ready_sem, inc=1, device_id=target(step), device_id_type=MESH)

    col_copy.wait()
    count_copy.wait()
    frac_copy.wait()
    for offset in range(num_off):
        if offset != reach:
            weight_copy(first_part(offset), first_weight.at[offset]).wait()
    for piece in range(pieces):
        flux_copy(piece).wait()
        lines = pl.ds(piece * PIECE, PIECE)
        for off in list(range(reach, 0, -1)) + list(range(-reach, 0)):
            block = col_ref[off + reach, 0, 0]
            frac = frac_ref[block]
            picked = merge_piece(block, piece, frac, jnp.sum(frac, axis=0, keepdims=True))
            staged_ref[off + reach, 0, lines, :] = product(picked.astype(jnp.bfloat16), off + reach, 0)
        for off in range(reach, 0, -1):
            remote(
                (off + reach, 0, lines), off, first_send.at[2 * (reach - off)], first_recv.at[2 * (reach - off)]
            ).start()
        if piece == pieces // 2:
            for turn in range(others):
                rest_copy(offset_of(turn) + reach).start()
            rest_copy(reach).start()

    rows_copy.wait()
    slot_ids = lax.broadcasted_iota(jnp.int32, (1, slots), 1)
    for offset in range(num_off):
        live_rows_ref[offset] = jnp.where(slot_ids < count_ref[0, offset], rows_ref[offset], -1)

    @pl.loop(0, land_blocks)
    def _(block):
        merged_ref[block] = merge(block)

    pl.semaphore_wait(ready_sem, reach)
    for turn in range(1, others, 2):
        first_copy(turn).start()
    for off in range(-reach, reach + 1):
        if off:
            table_copy(off).start()

    @pl.loop(0, sends)
    def _(i):
        chunk, off = plan(i)

        @pl.when(i < others)
        def _():
            rest_copy(off + reach).wait()

        multiply_chunk(chunk, off + reach)

        relayed = jnp.logical_and(is_source, i == RELAYED + 1)

        @pl.when(jnp.logical_and(jnp.logical_and(i > 0, i <= early), jnp.logical_not(relayed)))
        def _():
            chunk_copy(i - 1).start()

        @pl.when(relayed)
        def _():
            pl.semaphore_wait(relay_ready, helpers)
            for helper in range(helpers):
                relay_copy(helper).start()

        @pl.when(jnp.logical_and(is_helper, i == HELP_AT))
        def _():
            relay_copy(0).wait_recv()
            pass_copy(my_column).start()

        @pl.when(i > early)
        def _():
            late_copy(i - 1 - early).start()

    own_table = pltpu.make_async_copy(live_rows_ref.at[reach], tables_hbm.at[reach], in_sem.at[0])
    own_table.start()
    weight_copy(first_part(reach), first_weight.at[reach]).wait()
    multiply(merged_ref[col_ref[reach, 0, 0]], reach, 0)
    late_copy(others - 1).start()

    rest_copy(reach).wait()

    @pl.loop(0, chunks)
    def _(chunk):
        multiply_chunk(chunk, reach)

    for off in range(-reach, reach + 1):
        if off:
            table_copy(off).wait()
    own_table.wait()
    all_tables = pltpu.make_async_copy(tables_hbm, table_ref, in_sem.at[1])
    all_tables.start()
    all_tables.wait()

    def accumulate(block, start, slots_in):
        total = start
        for ref, offset, slot in slots_in:
            here = table_ref[offset, 0, slot] == block
            value = ref[offset, slot]
            total = total + jnp.where(here, value, jnp.zeros_like(value))
        sums_ref[block] = total

    @pl.loop(0, atm_blocks)
    def _(block):
        accumulate(
            block,
            jnp.zeros(sums_ref.shape[1:], jnp.float32),
            [(staged_ref, reach, slot) for slot in range(slots)],
        )

    @pl.loop(0, others)
    def _(turn):
        first_copy(turn).wait()

    @pl.loop(0, atm_blocks)
    def _(block):
        accumulate(
            block, sums_ref[block], [(arrived_ref, offset, 0) for offset in range(num_off) if offset != reach]
        )

    @pl.loop(0, chunks - 1)
    def _(chunk):
        @pl.loop(0, others)
        def _(turn):
            @pl.when(jnp.logical_not(jnp.logical_and(is_receiver, chunk * others + turn == RELAYED)))
            def _():
                chunk_copy(chunk * others + turn).wait_recv()

        @pl.when(jnp.logical_and(is_receiver, chunk == 0))
        def _():
            for helper in range(helpers):
                pass_copy(helper).wait_recv()

        @pl.loop(0, atm_blocks)
        def _(block):
            accumulate(
                block,
                sums_ref[block],
                [
                    (arrived_ref, offset, 1 + chunk * CHUNK + step)
                    for offset in range(num_off)
                    if offset != reach
                    for step in range(CHUNK)
                ],
            )

    @pl.loop(0, atm_blocks, unroll=2)
    def _(block):
        cells = pl.ds(pl.multiple_of(block * block_rows, block_rows), block_rows)
        for kind in range(num_kind):
            total_ref[kind, :, cells] = sums_ref[block, pl.ds(kind * num_step, num_step), :]

    total_out = pltpu.make_async_copy(total_ref, total_hbm, total_sem)
    total_out.start()

    @pl.loop(0, early)
    def _(i):
        @pl.when(jnp.logical_not(jnp.logical_and(is_source, i == RELAYED)))
        def _():
            chunk_copy(i).wait_send()

    @pl.when(is_source)
    def _():
        for helper in range(helpers):
            relay_copy(helper).wait_send()

    @pl.when(is_helper)
    def _():
        pass_copy(my_column).wait_send()

    total_out.wait()

    @pl.loop(0, others)
    def _(turn):
        late_copy(turn).wait()


def settle_kernel(table_hbm, late_ref, total_ref, out_hbm, out_ref, touched_ref, table_ref, out_sem, table_sem, block_sem):
    others, steps, _, block_rows = late_ref.shape
    num_kind, num_step, cells_dev = out_ref.shape
    atm_blocks = cells_dev // block_rows
    reach = others // 2
    first_slot = table_ref.shape[2] - steps

    def cells_of(block):
        return pl.ds(pl.multiple_of(block * block_rows, block_rows), block_rows)

    table_copy = pltpu.make_async_copy(table_hbm, table_ref, table_sem)
    table_copy.start()
    whole = pltpu.make_async_copy(total_ref, out_hbm, out_sem)
    for first in range(0, num_kind, num_kind // PARTS):
        kinds = pl.ds(first, num_kind // PARTS)
        pltpu.make_async_copy(total_ref.at[kinds], out_hbm.at[kinds], out_sem).start()
    table_copy.wait()

    arrivals = []
    for turn in range(others):
        offset = (reach - turn // 2) * (1 - 2 * (turn % 2)) + reach
        arrivals += [(turn, step, offset) for step in range(steps)]

    live = 0
    for turn, step, offset in arrivals:
        live = live + jnp.where(table_ref[offset, 0, first_slot + step] >= 0, 1, 0)

    @pl.when(live > 0)
    def _():
        @pl.loop(0, atm_blocks, unroll=8)
        def _(block):
            touched_ref[block] = 0

        for turn, step, offset in arrivals:
            row = table_ref[offset, 0, first_slot + step]

            @pl.when(row >= 0)
            def _():
                block = jnp.maximum(row, 0)
                cells = cells_of(block)
                fresh = touched_ref[block] == 0
                touched_ref[block] = 1

                @pl.when(fresh)
                def _():
                    for kind in range(num_kind):
                        out_ref[kind, :, cells] = (
                            total_ref[kind, :, cells] + late_ref[turn, step, pl.ds(kind * num_step, num_step), :]
                        )

                @pl.when(jnp.logical_not(fresh))
                def _():
                    for kind in range(num_kind):
                        out_ref[kind, :, cells] = (
                            out_ref[kind, :, cells] + late_ref[turn, step, pl.ds(kind * num_step, num_step), :]
                        )

    whole.wait()

    @pl.when(live > 0)
    def _():
        def rewrite(block):
            cells = cells_of(block)
            return pltpu.make_async_copy(out_ref.at[:, :, cells], out_hbm.at[:, :, cells], block_sem.at[block])

        @pl.loop(0, atm_blocks)
        def _(block):
            @pl.when(touched_ref[block] == 1)
            def _():
                rewrite(block).start()

        @pl.loop(0, atm_blocks)
        def _(block):
            @pl.when(touched_ref[block] == 1)
            def _():
                rewrite(block).wait()


def on_device(sizes, tile_flux, tile_frac, weights, block_row, block_col, send_counts):
    num_step, num_kind, tiles, cells = tile_flux.shape
    num_off, slots, block_rows, block_cols = weights.shape[1:]
    lines = num_step * num_kind
    chunks = (slots - 1) // CHUNK
    sends = chunks * (num_off - 1)
    tile_flux = tile_flux.reshape(num_step, num_kind, tiles, -1, block_cols).transpose(0, 1, 3, 2, 4)
    tile_frac = tile_frac.reshape(tiles, -1, block_cols).transpose(1, 0, 2)
    late, total, tables = pl.pallas_call(
        functools.partial(send_kernel, sizes),
        out_shape=(
            jax.ShapeDtypeStruct((num_off - 1, CHUNK, lines, block_rows), jnp.float32),
            jax.ShapeDtypeStruct((num_kind, num_step, AB_DEV * block_rows), jnp.float32),
            jax.ShapeDtypeStruct((num_off, 1, slots), jnp.int32),
        ),
        in_specs=[pl.BlockSpec(memory_space=pltpu.HBM)] * 6,
        out_specs=(pl.BlockSpec(memory_space=pl.ANY),) * 3,
        scratch_shapes=[
            [pltpu.VMEM((num_step, PIECE // num_step) + tile_flux.shape[2:], jnp.bfloat16)] * (lines // PIECE),
            pltpu.VMEM(tile_frac.shape, jnp.float32),
            pltpu.VMEM(weights.shape[1:], jnp.bfloat16),
            pltpu.VMEM((cells // block_cols, lines, block_cols), jnp.bfloat16),
            pltpu.VMEM((num_off, slots, lines, block_rows), jnp.float32),
            pltpu.VMEM((num_off, slots, lines, block_rows), jnp.float32),
            pltpu.VMEM((AB_DEV, lines, block_rows), jnp.float32),
            pltpu.VMEM((num_kind, num_step, AB_DEV * block_rows), jnp.float32),
            pltpu.SMEM((num_off, 1, slots), jnp.int32),
            pltpu.SMEM((1, num_off), jnp.int32),
            pltpu.SMEM((num_off, 1, slots), jnp.int32),
            pltpu.VMEM((num_off, 1, slots), jnp.int32),
            pltpu.VMEM((num_off, 1, slots), jnp.int32),
            pltpu.SemaphoreType.DMA((lines // PIECE + 4,)),
            pltpu.SemaphoreType.DMA((num_off,)),
            pltpu.SemaphoreType.DMA((num_off,)),
            pltpu.SemaphoreType.DMA,
            pltpu.SemaphoreType.DMA((num_off - 1,)),
            pltpu.SemaphoreType.DMA((num_off - 1,)),
            pltpu.SemaphoreType.DMA((sends,)),
            pltpu.SemaphoreType.DMA((sends,)),
            pltpu.SemaphoreType.DMA((num_off,)),
            pltpu.SemaphoreType.DMA((num_off,)),
            pltpu.SemaphoreType.REGULAR,
            pltpu.VMEM((lines, block_rows), jnp.float32),
            pltpu.SemaphoreType.REGULAR,
            pltpu.SemaphoreType.DMA((CHUNK,)),
            pltpu.SemaphoreType.DMA,
            pltpu.SemaphoreType.DMA,
            pltpu.SemaphoreType.DMA((CHUNK,)),
        ],
        compiler_params=pltpu.CompilerParams(
            collective_id=0, has_side_effects=True, vmem_limit_bytes=40 * 1024 * 1024
        ),
    )(*(
        pltpu.with_memory_space_constraint(value, pltpu.HBM)
        for value in (tile_flux, tile_frac, weights[0], block_row.transpose(1, 0, 2), block_col.transpose(1, 0, 2), send_counts)
    ))
    settled = pl.pallas_call(
        settle_kernel,
        out_shape=jax.ShapeDtypeStruct((num_kind, num_step, AB_DEV * block_rows), jnp.float32),
        in_specs=[pl.BlockSpec(memory_space=pl.ANY)] + [pl.BlockSpec(memory_space=pltpu.VMEM)] * 2,
        out_specs=pl.BlockSpec(memory_space=pltpu.HBM),
        scratch_shapes=[
            pltpu.VMEM((num_kind, num_step, AB_DEV * block_rows), jnp.float32),
            pltpu.SMEM((AB_DEV,), jnp.int32),
            pltpu.SMEM((num_off, 1, slots), jnp.int32),
            pltpu.SemaphoreType.DMA,
            pltpu.SemaphoreType.DMA,
            pltpu.SemaphoreType.DMA((AB_DEV,)),
        ],
        compiler_params=pltpu.CompilerParams(vmem_limit_bytes=12 * 1024 * 1024),
    )(tables, late, total)
    return settled.transpose(1, 0, 2)


def solution(mesh):
    sizes = (mesh.shape["gx"], mesh.shape["gy"])
    return jax.shard_map(
        functools.partial(on_device, sizes),
        mesh=mesh,
        in_specs=(
            P(None, None, None, ("gx", "gy")),
            P(None, ("gx", "gy")),
            P(("gx", "gy"), None, None, None, None),
            P(("gx", "gy"), None, None),
            P(("gx", "gy"), None, None),
            P(("gx", "gy"), None),
        ),
        out_specs=P(None, None, ("gx", "gy")),
        check_vma=False,
    )
```

```python
import functools

import jax
import jax.numpy as jnp
from jax import lax
from jax.experimental import pallas as pl
from jax.experimental.pallas import tpu as pltpu
from jax.sharding import PartitionSpec as P

MESH = pl.DeviceIdType.MESH
AB_DEV = 48
PARTS = 4
CHUNK = 3
PIECE = 8
COLUMN = 16
RELAYED = 2
HELP_AT = 10


def combine(a, b, shift, mask):
    return jnp.where(mask, a + pltpu.roll(a, 8 - shift, 0), b + pltpu.roll(b, shift, 0))


def sum_rows(parts):
    row = lax.broadcasted_iota(jnp.int32, (8, 128), 0)
    top = [combine(parts[r], parts[r + 4], 4, row < 4) for r in range(4)]
    mid = [combine(top[r], top[r + 2], 2, (row & 2) == 0) for r in range(2)]
    return combine(mid[0], mid[1], 1, (row & 1) == 0)


def send_kernel(
    sizes,
    flux_hbm, frac_hbm, weights_hbm, rows_hbm, col_hbm, count_hbm,
    late_hbm, total_hbm, tables_hbm,
    flux_refs, frac_ref, weights_ref, merged_ref, staged_ref, arrived_ref, sums_ref, total_ref,
    col_ref, count_ref, table_ref, rows_ref, live_rows_ref,
    in_sem, first_weight, weight_sem, total_sem, first_send, first_recv, send_sem, recv_sem, table_send, table_recv, ready_sem,
    relay_ref, relay_ready, relay_send, relay_recv, pass_send, pass_recv,
):
    num_x, num_y = sizes
    devices = num_x * num_y
    pieces = len(flux_refs)
    num_step, piece_kinds = flux_refs[0].shape[:2]
    num_kind = pieces * piece_kinds
    num_off, slots = weights_ref.shape[:2]
    reach = num_off // 2
    others = num_off - 1
    land_blocks = merged_ref.shape[0]
    chunks = (slots - 1) // CHUNK
    sends = chunks * others
    early = sends - others
    atm_blocks = sums_ref.shape[0]
    block_rows = staged_ref.shape[3]
    me = lax.axis_index("gx") * num_y + lax.axis_index("gy")

    columns = num_y // COLUMN
    my_column = lax.axis_index("gy") // COLUMN
    my_chip = lax.axis_index("gy") % COLUMN // 2
    at_end = my_chip == COLUMN // 2 - 1
    is_source = jnp.logical_and(at_end, my_column == columns - 1)
    is_helper = jnp.logical_and(at_end, my_column < columns - 1)
    is_receiver = jnp.logical_and(my_chip == 0, my_column == 0)
    helpers = columns - 1
    assert helpers == CHUNK

    def flux_copy(piece):
        kinds = pl.ds(piece * piece_kinds, piece_kinds)
        return pltpu.make_async_copy(flux_hbm.at[:, kinds], flux_refs[piece], in_sem.at[piece])

    def offset_of(turn):
        return (reach - turn // 2) * (1 - 2 * (turn % 2))

    swap = jnp.where(is_helper, 2, 0)

    def order(i):
        pair = i % others // 2
        return i + swap * (pair % 2 - pair // 2)

    def plan(i):
        return i // others, offset_of(i % others)

    def chunk_part(chunk, offset):
        return offset, pl.ds(1 + chunk * CHUNK, CHUNK)

    def weight_copy(part, sem):
        return pltpu.make_async_copy(weights_hbm.at[part], weights_ref.at[part], sem)

    def first_part(offset):
        return offset, pl.ds(0, 1)

    def rest_copy(offset):
        return weight_copy((offset, pl.ds(1, slots - 1)), weight_sem.at[offset])

    def target(off):
        there = (me + off + devices) % devices
        return (there // num_y, there % num_y)

    relay_off = 2
    relay_at = relay_off + reach

    def relay_copy(helper):
        return pltpu.make_async_remote_copy(
            src_ref=staged_ref.at[relay_at, 1 + helper],
            dst_ref=relay_ref,
            send_sem=relay_send.at[helper],
            recv_sem=relay_recv,
            device_id=target(-COLUMN * (helpers - helper)),
            device_id_type=MESH,
        )

    def pass_copy(helper):
        return pltpu.make_async_remote_copy(
            src_ref=relay_ref,
            dst_ref=arrived_ref.at[relay_at, 1 + helper],
            send_sem=pass_send,
            recv_sem=pass_recv.at[helper],
            device_id=target(COLUMN * (helpers - helper) + relay_off),
            device_id_type=MESH,
        )

    barrier = pltpu.get_barrier_semaphore()
    for step in range(1, reach + 1):
        pl.semaphore_signal(barrier, inc=1, device_id=target(-step), device_id_type=MESH)

    @pl.when(is_source)
    def _():
        for helper in range(helpers):
            pl.semaphore_signal(
                barrier, inc=1, device_id=target(-COLUMN * (helpers - helper)), device_id_type=MESH
            )

    @pl.when(is_receiver)
    def _():
        for helper in range(helpers):
            pl.semaphore_signal(
                barrier, inc=1, device_id=target(-relay_off - COLUMN * (helpers - helper)), device_id_type=MESH
            )

    col_copy = pltpu.make_async_copy(col_hbm, col_ref, in_sem.at[pieces + 1])
    count_copy = pltpu.make_async_copy(count_hbm, count_ref, in_sem.at[pieces + 2])
    frac_copy = pltpu.make_async_copy(frac_hbm, frac_ref, in_sem.at[pieces])
    rows_copy = pltpu.make_async_copy(rows_hbm, rows_ref, in_sem.at[pieces + 3])
    col_copy.start()
    count_copy.start()
    frac_copy.start()
    for offset in range(num_off):
        weight_copy(first_part(offset), first_weight.at[offset]).start()
    for piece in range(pieces):
        flux_copy(piece).start()
    rows_copy.start()

    def merge_piece(block, piece, frac, total):
        parts = []
        for line in range(PIECE):
            kind, step = line // num_step, line % num_step
            parts.append(flux_refs[piece][step, kind, block].astype(jnp.float32) * frac)
        return sum_rows(parts) / total

    def merge(block):
        frac = frac_ref[block]
        total = jnp.sum(frac, axis=0, keepdims=True)
        return jnp.concatenate(
            [merge_piece(block, piece, frac, total) for piece in range(pieces)], axis=0
        ).astype(jnp.bfloat16)

    def table_copy(off):
        return pltpu.make_async_remote_copy(
            src_ref=live_rows_ref.at[off + reach],
            dst_ref=tables_hbm.at[off + reach],
            send_sem=table_send.at[off + reach],
            recv_sem=table_recv.at[off + reach],
            device_id=target(off),
            device_id_type=MESH,
        )

    def remote(part, off, to_sem, from_sem):
        return pltpu.make_async_remote_copy(
            src_ref=staged_ref.at[part],
            dst_ref=arrived_ref.at[part],
            send_sem=to_sem,
            recv_sem=from_sem,
            device_id=target(off),
            device_id_type=MESH,
        )

    def first_copy(turn):
        off = offset_of(turn)
        return remote(first_part(off + reach), off, first_send.at[turn], first_recv.at[turn])

    def chunk_copy(i):
        chunk, off = plan(i)
        return remote(chunk_part(chunk, off + reach), off, send_sem.at[i], recv_sem.at[i])

    def late_copy(turn):
        off = offset_of(turn)
        return pltpu.make_async_remote_copy(
            src_ref=staged_ref.at[chunk_part(chunks - 1, off + reach)],
            dst_ref=late_hbm.at[turn],
            send_sem=send_sem.at[early + turn],
            recv_sem=recv_sem.at[early + turn],
            device_id=target(off),
            device_id_type=MESH,
        )

    def product(picked, offset, slot):
        picked = jnp.where(slot < count_ref[0, offset], picked, jnp.zeros_like(picked))
        return lax.dot_general(
            picked, weights_ref[offset, slot], (((1,), (1,)), ((), ())),
            preferred_element_type=jnp.float32,
        )

    def multiply(picked, offset, slot):
        staged_ref[offset, slot] = product(picked, offset, slot)

    def multiply_chunk(chunk, offset):
        for step in range(CHUNK):
            slot = 1 + chunk * CHUNK + step
            multiply(merged_ref[col_ref[offset, 0, slot]], offset, slot)

    @pl.when(jnp.logical_not(is_helper))
    def _():
        pl.semaphore_wait(barrier, reach)

    @pl.when(is_helper)
    def _():
        pl.semaphore_wait(barrier, reach + 2)
        pl.semaphore_signal(
            relay_ready, inc=1, device_id=target(COLUMN * (helpers - my_column)), device_id_type=MESH
        )

    for step in range(1, reach + 1):
        pl.semaphore_signal(ready_sem, inc=1, device_id=target(step), device_id_type=MESH)

    col_copy.wait()
    count_copy.wait()
    frac_copy.wait()
    for offset in range(num_off):
        if offset != reach:
            weight_copy(first_part(offset), first_weight.at[offset]).wait()
    for piece in range(pieces):
        flux_copy(piece).wait()
        lines = pl.ds(piece * PIECE, PIECE)
        for off in list(range(reach, 0, -1)) + list(range(-reach, 0)):
            block = col_ref[off + reach, 0, 0]
            frac = frac_ref[block]
            picked = merge_piece(block, piece, frac, jnp.sum(frac, axis=0, keepdims=True))
            staged_ref[off + reach, 0, lines, :] = product(picked.astype(jnp.bfloat16), off + reach, 0)
        for off in range(reach, 0, -1):
            remote(
                (off + reach, 0, lines), off, first_send.at[2 * (reach - off)], first_recv.at[2 * (reach - off)]
            ).start()
        if piece == pieces // 2:
            for turn in range(others):
                rest_copy(offset_of(turn) + reach).start()
            rest_copy(reach).start()

    rows_copy.wait()
    slot_ids = lax.broadcasted_iota(jnp.int32, (1, slots), 1)
    for offset in range(num_off):
        live_rows_ref[offset] = jnp.where(slot_ids < count_ref[0, offset], rows_ref[offset], -1)

    @pl.loop(0, land_blocks)
    def _(block):
        merged_ref[block] = merge(block)

    pl.semaphore_wait(ready_sem, reach)
    for turn in range(1, others, 2):
        first_copy(turn).start()
    for off in range(-reach, reach + 1):
        if off:
            table_copy(off).start()

    @pl.loop(0, sends)
    def _(i):
        chunk, off = plan(order(i))

        @pl.when(i < others)
        def _():
            rest_copy(off + reach).wait()

        multiply_chunk(chunk, off + reach)

        relayed = jnp.logical_and(is_source, i == RELAYED + 1)

        @pl.when(jnp.logical_and(jnp.logical_and(i > 0, i <= early), jnp.logical_not(relayed)))
        def _():
            chunk_copy(order(i - 1)).start()

        @pl.when(relayed)
        def _():
            pl.semaphore_wait(relay_ready, helpers)
            for helper in range(helpers):
                relay_copy(helper).start()

        @pl.when(jnp.logical_and(is_helper, i == HELP_AT))
        def _():
            relay_copy(0).wait_recv()
            pass_copy(my_column).start()

        @pl.when(i > early)
        def _():
            late_copy(order(i - 1) - early).start()

    own_table = pltpu.make_async_copy(live_rows_ref.at[reach], tables_hbm.at[reach], in_sem.at[0])
    own_table.start()
    weight_copy(first_part(reach), first_weight.at[reach]).wait()
    multiply(merged_ref[col_ref[reach, 0, 0]], reach, 0)
    late_copy(order(sends - 1) - early).start()

    rest_copy(reach).wait()

    @pl.loop(0, chunks)
    def _(chunk):
        multiply_chunk(chunk, reach)

    for off in range(-reach, reach + 1):
        if off:
            table_copy(off).wait()
    own_table.wait()
    all_tables = pltpu.make_async_copy(tables_hbm, table_ref, in_sem.at[1])
    all_tables.start()
    all_tables.wait()

    def accumulate(block, start, slots_in):
        total = start
        for ref, offset, slot in slots_in:
            here = table_ref[offset, 0, slot] == block
            value = ref[offset, slot]
            total = total + jnp.where(here, value, jnp.zeros_like(value))
        sums_ref[block] = total

    @pl.loop(0, atm_blocks)
    def _(block):
        accumulate(
            block,
            jnp.zeros(sums_ref.shape[1:], jnp.float32),
            [(staged_ref, reach, slot) for slot in range(slots)],
        )

    @pl.loop(0, others)
    def _(turn):
        first_copy(turn).wait()

    @pl.loop(0, atm_blocks)
    def _(block):
        accumulate(
            block, sums_ref[block], [(arrived_ref, offset, 0) for offset in range(num_off) if offset != reach]
        )

    @pl.loop(0, chunks - 1)
    def _(chunk):
        @pl.loop(0, others)
        def _(turn):
            @pl.when(jnp.logical_not(jnp.logical_and(is_receiver, chunk * others + turn == RELAYED)))
            def _():
                chunk_copy(chunk * others + turn).wait_recv()

        @pl.when(jnp.logical_and(is_receiver, chunk == 0))
        def _():
            for helper in range(helpers):
                pass_copy(helper).wait_recv()

        @pl.loop(0, atm_blocks)
        def _(block):
            accumulate(
                block,
                sums_ref[block],
                [
                    (arrived_ref, offset, 1 + chunk * CHUNK + step)
                    for offset in range(num_off)
                    if offset != reach
                    for step in range(CHUNK)
                ],
            )

    @pl.loop(0, atm_blocks, unroll=2)
    def _(block):
        cells = pl.ds(pl.multiple_of(block * block_rows, block_rows), block_rows)
        for kind in range(num_kind):
            total_ref[kind, :, cells] = sums_ref[block, pl.ds(kind * num_step, num_step), :]

    total_out = pltpu.make_async_copy(total_ref, total_hbm, total_sem)
    total_out.start()

    @pl.loop(0, early)
    def _(i):
        @pl.when(jnp.logical_not(jnp.logical_and(is_source, i == RELAYED)))
        def _():
            chunk_copy(i).wait_send()

    @pl.when(is_source)
    def _():
        for helper in range(helpers):
            relay_copy(helper).wait_send()

    @pl.when(is_helper)
    def _():
        pass_copy(my_column).wait_send()

    total_out.wait()

    @pl.loop(0, others)
    def _(turn):
        late_copy(turn).wait()


def settle_kernel(table_hbm, late_ref, total_ref, out_hbm, out_ref, touched_ref, table_ref, out_sem, table_sem, block_sem):
    others, steps, _, block_rows = late_ref.shape
    num_kind, num_step, cells_dev = out_ref.shape
    atm_blocks = cells_dev // block_rows
    reach = others // 2
    first_slot = table_ref.shape[2] - steps

    def cells_of(block):
        return pl.ds(pl.multiple_of(block * block_rows, block_rows), block_rows)

    table_copy = pltpu.make_async_copy(table_hbm, table_ref, table_sem)
    table_copy.start()
    whole = pltpu.make_async_copy(total_ref, out_hbm, out_sem)
    for first in range(0, num_kind, num_kind // PARTS):
        kinds = pl.ds(first, num_kind // PARTS)
        pltpu.make_async_copy(total_ref.at[kinds], out_hbm.at[kinds], out_sem).start()
    table_copy.wait()

    arrivals = []
    for turn in range(others):
        offset = (reach - turn // 2) * (1 - 2 * (turn % 2)) + reach
        arrivals += [(turn, step, offset) for step in range(steps)]

    live = 0
    for turn, step, offset in arrivals:
        live = live + jnp.where(table_ref[offset, 0, first_slot + step] >= 0, 1, 0)

    @pl.when(live > 0)
    def _():
        @pl.loop(0, atm_blocks, unroll=8)
        def _(block):
            touched_ref[block] = 0

        for turn, step, offset in arrivals:
            row = table_ref[offset, 0, first_slot + step]

            @pl.when(row >= 0)
            def _():
                block = jnp.maximum(row, 0)
                cells = cells_of(block)
                fresh = touched_ref[block] == 0
                touched_ref[block] = 1

                @pl.when(fresh)
                def _():
                    for kind in range(num_kind):
                        out_ref[kind, :, cells] = (
                            total_ref[kind, :, cells] + late_ref[turn, step, pl.ds(kind * num_step, num_step), :]
                        )

                @pl.when(jnp.logical_not(fresh))
                def _():
                    for kind in range(num_kind):
                        out_ref[kind, :, cells] = (
                            out_ref[kind, :, cells] + late_ref[turn, step, pl.ds(kind * num_step, num_step), :]
                        )

    whole.wait()

    @pl.when(live > 0)
    def _():
        def rewrite(block):
            cells = cells_of(block)
            return pltpu.make_async_copy(out_ref.at[:, :, cells], out_hbm.at[:, :, cells], block_sem.at[block])

        @pl.loop(0, atm_blocks)
        def _(block):
            @pl.when(touched_ref[block] == 1)
            def _():
                rewrite(block).start()

        @pl.loop(0, atm_blocks)
        def _(block):
            @pl.when(touched_ref[block] == 1)
            def _():
                rewrite(block).wait()


def on_device(sizes, tile_flux, tile_frac, weights, block_row, block_col, send_counts):
    num_step, num_kind, tiles, cells = tile_flux.shape
    num_off, slots, block_rows, block_cols = weights.shape[1:]
    lines = num_step * num_kind
    chunks = (slots - 1) // CHUNK
    sends = chunks * (num_off - 1)
    tile_flux = tile_flux.reshape(num_step, num_kind, tiles, -1, block_cols).transpose(0, 1, 3, 2, 4)
    tile_frac = tile_frac.reshape(tiles, -1, block_cols).transpose(1, 0, 2)
    late, total, tables = pl.pallas_call(
        functools.partial(send_kernel, sizes),
        out_shape=(
            jax.ShapeDtypeStruct((num_off - 1, CHUNK, lines, block_rows), jnp.float32),
            jax.ShapeDtypeStruct((num_kind, num_step, AB_DEV * block_rows), jnp.float32),
            jax.ShapeDtypeStruct((num_off, 1, slots), jnp.int32),
        ),
        in_specs=[pl.BlockSpec(memory_space=pltpu.HBM)] * 6,
        out_specs=(pl.BlockSpec(memory_space=pl.ANY),) * 3,
        scratch_shapes=[
            [pltpu.VMEM((num_step, PIECE // num_step) + tile_flux.shape[2:], jnp.bfloat16)] * (lines // PIECE),
            pltpu.VMEM(tile_frac.shape, jnp.float32),
            pltpu.VMEM(weights.shape[1:], jnp.bfloat16),
            pltpu.VMEM((cells // block_cols, lines, block_cols), jnp.bfloat16),
            pltpu.VMEM((num_off, slots, lines, block_rows), jnp.float32),
            pltpu.VMEM((num_off, slots, lines, block_rows), jnp.float32),
            pltpu.VMEM((AB_DEV, lines, block_rows), jnp.float32),
            pltpu.VMEM((num_kind, num_step, AB_DEV * block_rows), jnp.float32),
            pltpu.SMEM((num_off, 1, slots), jnp.int32),
            pltpu.SMEM((1, num_off), jnp.int32),
            pltpu.SMEM((num_off, 1, slots), jnp.int32),
            pltpu.VMEM((num_off, 1, slots), jnp.int32),
            pltpu.VMEM((num_off, 1, slots), jnp.int32),
            pltpu.SemaphoreType.DMA((lines // PIECE + 4,)),
            pltpu.SemaphoreType.DMA((num_off,)),
            pltpu.SemaphoreType.DMA((num_off,)),
            pltpu.SemaphoreType.DMA,
            pltpu.SemaphoreType.DMA((num_off - 1,)),
            pltpu.SemaphoreType.DMA((num_off - 1,)),
            pltpu.SemaphoreType.DMA((sends,)),
            pltpu.SemaphoreType.DMA((sends,)),
            pltpu.SemaphoreType.DMA((num_off,)),
            pltpu.SemaphoreType.DMA((num_off,)),
            pltpu.SemaphoreType.REGULAR,
            pltpu.VMEM((lines, block_rows), jnp.float32),
            pltpu.SemaphoreType.REGULAR,
            pltpu.SemaphoreType.DMA((CHUNK,)),
            pltpu.SemaphoreType.DMA,
            pltpu.SemaphoreType.DMA,
            pltpu.SemaphoreType.DMA((CHUNK,)),
        ],
        compiler_params=pltpu.CompilerParams(
            collective_id=0, has_side_effects=True, vmem_limit_bytes=40 * 1024 * 1024
        ),
    )(*(
        pltpu.with_memory_space_constraint(value, pltpu.HBM)
        for value in (tile_flux, tile_frac, weights[0], block_row.transpose(1, 0, 2), block_col.transpose(1, 0, 2), send_counts)
    ))
    settled = pl.pallas_call(
        settle_kernel,
        out_shape=jax.ShapeDtypeStruct((num_kind, num_step, AB_DEV * block_rows), jnp.float32),
        in_specs=[pl.BlockSpec(memory_space=pl.ANY)] + [pl.BlockSpec(memory_space=pltpu.VMEM)] * 2,
        out_specs=pl.BlockSpec(memory_space=pltpu.HBM),
        scratch_shapes=[
            pltpu.VMEM((num_kind, num_step, AB_DEV * block_rows), jnp.float32),
            pltpu.SMEM((AB_DEV,), jnp.int32),
            pltpu.SMEM((num_off, 1, slots), jnp.int32),
            pltpu.SemaphoreType.DMA,
            pltpu.SemaphoreType.DMA,
            pltpu.SemaphoreType.DMA((AB_DEV,)),
        ],
        compiler_params=pltpu.CompilerParams(vmem_limit_bytes=12 * 1024 * 1024),
    )(tables, late, total)
    return settled.transpose(1, 0, 2)


def solution(mesh):
    sizes = (mesh.shape["gx"], mesh.shape["gy"])
    return jax.shard_map(
        functools.partial(on_device, sizes),
        mesh=mesh,
        in_specs=(
            P(None, None, None, ("gx", "gy")),
            P(None, ("gx", "gy")),
            P(("gx", "gy"), None, None, None, None),
            P(("gx", "gy"), None, None),
            P(("gx", "gy"), None, None),
            P(("gx", "gy"), None),
        ),
        out_specs=P(None, None, ("gx", "gy")),
        check_vma=False,
    )
```
